256 devices in a mesh: space: 4 (over z_hi, core), fsdp: 64 (over y, x, z_lo).
Axes of the slice: x: 4, y: 4, z: 8 (z_hi: 2, z_lo: 4; z = z_hi * 4 + z_lo), core: 2. Of those that a mesh axis runs over, the one named last changes fastest.
Arguments:
- acts: bfloat16 [64, 8, 16, 16, 512], P('fsdp', 'space'), may hold values from -16 to 16
- kernel: bfloat16 [512, 27, 256], P('fsdp'), may hold values from -0.0546875 to 0.0546875
- cotangent: bfloat16 [64, 8, 16, 16, 256], P('fsdp', 'space'), may hold values from -6 to 6
Outputs:
- outputs: bfloat16 [64, 8, 16, 16, 256], P('fsdp', 'space')
- grad_input: bfloat16 [64, 8, 16, 16, 512], P('fsdp', 'space')
- grad_kernel: float32 [512, 27, 256], P('fsdp')
The draws below stay inside these ranges and needn't reach their ends.
All inputs are finite; a program needn't handle non-finite values.
Results may differ from the reference program's by a relative error of at most 0.0095.
Values may be sent and summed in bfloat16 or wider, within the bound.
A program may use at most 128 MiB of HBM per device.

```python
import jax
import jax.numpy as jnp
from jax import lax

C_IN = 512
C_OUT = 256
TAPS = 27
SIDE = 16
SAMPLES = 64
DEPTH = 8


def spiked(entries, key, source, target, shards_of, factor):
    def block_of(dim):
        return (jnp.arange(entries.shape[dim]) // (entries.shape[dim] // shards_of)).reshape((-1,) + (1,) * (entries.ndim - 1 - dim))

    near = jax.random.permutation(key, shards_of)[block_of(target)]
    second = (block_of(target) + shards_of // 2) % shards_of
    return jnp.where((block_of(source) == near) | (block_of(source) == second), factor * entries, entries)


def block_levels(stream_key, dims, shards, least, top_value):
    def one(dim, shards_of):
        draws = jax.random.uniform(jax.random.fold_in(jax.random.fold_in(stream_key, 6), dim), (shards_of,), jnp.float32, least / len(shards), top_value / len(shards))
        return jnp.repeat(jnp.exp(draws), dims[dim] // shards_of).reshape((-1,) + (1,) * (len(dims) - dim - 1))

    level = one(*shards[0])
    for cut in shards[1:]:
        level = level * one(*cut)
    return level


def gaussian(own_key, extent, scale, limit, cuts=(), held_as=jnp.bfloat16):
    values = jax.random.normal(own_key, extent, jnp.float32) * scale
    if len(cuts) > 0:
        values = block_levels(own_key, extent, cuts, -0.22, 0.18) * values
    return jnp.clip(values, min=-limit, max=limit).astype(held_as)


def heavy_noise(stream_key, shape, width, reach, split, heavy, dtype=jnp.bfloat16):
    values = width * jax.random.normal(stream_key, shape, jnp.float32)
    if split:
        values = values * block_levels(stream_key, shape, split, -0.22, 0.18)
    return jnp.clip(spiked(values, jax.random.fold_in(stream_key, 3), *heavy), -reach, reach).astype(dtype)


def setup_inputs(seed: int = 0) -> dict:
    arg_keys = jax.random.split(jax.random.key(seed), 4)
    acts = heavy_noise(arg_keys[0], (SAMPLES, DEPTH, SIDE, SIDE, C_IN), 1.0, 16.0, ((0, 64), (1, 4)), (0, 4, 64, 4.0))
    kernel = gaussian(arg_keys[1], (C_IN, TAPS, C_OUT), (TAPS * C_IN) ** -0.5, 0.0546875, ((0, 64),))
    cotangent = gaussian(arg_keys[2], (SAMPLES, DEPTH, SIDE, SIDE, C_OUT), 1.0, 6.0, ((0, 64), (1, 4)))
    return dict(acts=acts, kernel=kernel, cotangent=cotangent)


kernel_offsets = [(i // 9 - 1, (i // 3) % 3 - 1, i % 3 - 1) for i in range(27)]


def reference(acts, kernel, cotangent):
    cell_count = DEPTH * SIDE * SIDE
    widths = ((1, 1), (1, 1), (1, 1), (0, 0))

    def one_sample(running, inputs):
        sample_acts, sample_grad = inputs
        acts_float = sample_acts.astype(jnp.float32)
        squash = jax.nn.sigmoid(acts_float)
        hidden = (acts_float * squash).astype(jnp.bfloat16)
        hidden_pad = jnp.pad(hidden, widths)
        grad_pad = jnp.pad(sample_grad, widths)
        grad_flat = sample_grad.reshape(cell_count, C_OUT)
        result = jnp.zeros((cell_count, C_OUT), jnp.float32)
        back = jnp.zeros((cell_count, C_IN), jnp.float32)
        tap_grads = []
        for tap_index in range(TAPS):
            shift_d, shift_h, shift_w = kernel_offsets[tap_index]
            shifted = hidden_pad[1 + shift_d:1 + shift_d + DEPTH, 1 + shift_h:1 + shift_h + SIDE, 1 + shift_w:1 + shift_w + SIDE].reshape(cell_count, C_IN)
            shifted_grad = grad_pad[1 - shift_d:1 - shift_d + DEPTH, 1 - shift_h:1 - shift_h + SIDE, 1 - shift_w:1 - shift_w + SIDE].reshape(cell_count, C_OUT)
            tap_weight = kernel[:, tap_index, :]
            result = result + jnp.dot(shifted, tap_weight, preferred_element_type=jnp.float32)
            back = back + jnp.dot(shifted_grad, tap_weight.T, preferred_element_type=jnp.float32)
            tap_grads.append(lax.dot_general(shifted, grad_flat, (((0,), (0,)), ((), ())), preferred_element_type=jnp.float32))
        running = running + jnp.stack(tap_grads, axis=1)
        back = back.reshape(DEPTH, SIDE, SIDE, C_IN)
        grad_in = (back * squash * (1.0 + acts_float * (1.0 - squash))).astype(jnp.bfloat16)
        out_sample = result.astype(jnp.bfloat16).reshape(DEPTH, SIDE, SIDE, C_OUT)
        return running, (out_sample, grad_in)

    start_grad = jnp.zeros((C_IN, TAPS, C_OUT), jnp.float32)
    summed, (outputs, grad_input) = lax.scan(one_sample, start_grad, (acts, cotangent))
    grad_kernel = summed * (1.0 / SAMPLES)
    return outputs, grad_input, grad_kernel
```

```python
import functools

import jax
import jax.numpy as jnp
from jax import lax
from jax.experimental import pallas as pl
from jax.experimental.pallas import tpu as pltpu
from jax.sharding import PartitionSpec as P

MESH = pl.DeviceIdType.MESH
F32 = jnp.float32
BF16 = jnp.bfloat16
ORDERS = (("z", "x", "y"), ("y", "z", "x"), ("x", "y", "z"))
LOW, HIGH = pl.ds(0, 2), pl.ds(2, 2)
COPIES = 128


def silu(v):
    return v * jax.nn.sigmoid(v)


def step_kernel(
    acts,
    cot,
    shard,
    outputs,
    grad_input,
    grad_kernel,
    weights,
    partial,
    from_partner,
    rx3p,
    rx3m,
    rx2p,
    rx2m,
    rx1,
    own_sum,
    other_sum,
    final_own,
    final_other,
    hidden3,
    cot3,
    hidden_t,
    halo_acts,
    halo_cot,
    acc_out,
    acc_back,
    send_sem,
    recv_sem,
    local_sem,
):
    space, fsdp = lax.axis_index("space"), lax.axis_index("fsdp")
    core, z_hi = space % 2, space // 2
    y, x, zl = fsdp // 16, (fsdp // 4) % 4, fsdp % 4
    z = z_hi * 4 + zl
    own = {"y": y, "x": x, "z": zl}

    def neighbour(dim, delta):
        if dim == "y":
            return (space, ((y + 4 + delta) % 4) * 16 + x * 4 + zl)
        if dim == "x":
            return (space, y * 16 + ((x + 4 + delta) % 4) * 4 + zl)
        there = (z + 8 + delta) % 8
        return ((there // 4) * 2 + core, y * 16 + x * 4 + there % 4)

    partner = (z_hi * 2 + 1 - core, fsdp)
    across = ((space + 2) % 4, fsdp)
    greeted = [neighbour(d, k) for d in ("y", "x") for k in (1, -1, 2)]
    greeted += [neighbour("z", k) for k in (1, -1, 2, -2)]
    greeted += [partner, across, (3 - space, fsdp)]

    barrier = pltpu.get_barrier_semaphore()
    for device in greeted:
        pl.semaphore_signal(barrier, inc=1, device_id=device, device_id_type=MESH)
    pl.semaphore_wait(barrier, len(greeted))

    counter = [0]
    sent = []

    def remote(src, dst, device):
        number = counter[0]
        counter[0] += 1
        return pltpu.make_async_remote_copy(
            src_ref=src,
            dst_ref=dst,
            send_sem=send_sem.at[number],
            recv_sem=recv_sem.at[number],
            device_id=device,
            device_id_type=MESH,
        )

    def send(src, dst, device):
        copy = remote(src, dst, device)
        copy.start()
        sent.append(copy)
        return copy

    def at(dim, delta):
        return (own[dim] + 4 + delta) % 4

    def place(colour, first, second, third):
        d1, d2, d3 = ORDERS[colour]
        index = {d1: first, d2: second, d3: third}
        return index["y"], index["x"], index["z"]

    every = slice(None)

    halo_copies = []
    for src, dst in ((cot, halo_cot), (acts, halo_acts)):
        down = remote(src.at[0], dst.at[1], (space - 1, fsdp))
        up = remote(src.at[1], dst.at[0], (space + 1, fsdp))
        halo_copies.append((down, up))

    def each_halo(number, action_down, action_up):
        down, up = halo_copies[number]

        @pl.when(space > 0)
        def _():
            action_down(down, up)

        @pl.when(space < 3)
        def _():
            action_up(down, up)

    def start_halo(number):
        each_halo(number, lambda d, u: d.start(), lambda d, u: u.start())

    def take_halo(number):
        each_halo(number, lambda d, u: u.wait_recv(), lambda d, u: d.wait_recv())

    def end_halo(number):
        each_halo(number, lambda d, u: d.wait_send(), lambda d, u: u.wait_send())

    def slot(colour, first, second, third):
        iy, ix, iz = place(colour, first, second, third)
        return weights.at[core, pl.ds(9 * colour, 9), iy, ix, iz]

    waiting = {}

    def spread(key, colour, where, device):
        piece = slot(colour, *where)
        waiting.setdefault(key, []).append(send(piece, piece, device))

    def take(key):
        for copy in waiting.pop(key):
            copy.wait_recv()

    def gather_0():
        for colour, (d1, d2, d3) in enumerate(ORDERS):
            here = slot(colour, own[d1], own[d2], own[d3])
            for delta in (1, -1, 2):
                copy = send(shard.at[core, pl.ds(9 * colour, 9)], here, neighbour(d1, delta))
                waiting.setdefault("a1", []).append(copy)

    def gather_1():
        take("a1")
        for colour, (d1, d2, d3) in enumerate(ORDERS):
            for delta in (1, -1):
                spread("a2", colour, (every, own[d2], own[d3]), neighbour(d2, delta))

    def gather_2():
        take("a2")
        for colour, (d1, d2, d3) in enumerate(ORDERS):
            spread("a3", colour, (LOW, at(d2, -1), own[d3]), neighbour(d2, 1))
            spread("a3", colour, (HIGH, at(d2, 1), own[d3]), neighbour(d2, -1))

    def gather_3():
        take("a3")
        for colour, (d1, d2, d3) in enumerate(ORDERS):
            for delta in (1, -1):
                spread("a4", colour, (every, every, own[d3]), neighbour(d3, delta))
        for colour, (d1, d2, d3) in enumerate(ORDERS):
            spread("pair", colour, (every, every, own[d3]), partner)

    def gather_4():
        take("a4")
        for colour, (d1, d2, d3) in enumerate(ORDERS):
            spread("a5", colour, (LOW, every, at(d3, -1)), neighbour(d3, 1))
            spread("a5", colour, (HIGH, every, at(d3, 1)), neighbour(d3, -1))
        for colour, (d1, d2, d3) in enumerate(ORDERS):
            for delta in (1, -1):
                spread("pair", colour, (every, every, at(d3, delta)), partner)

    def gather_5():
        take("a5")
        for colour, (d1, d2, d3) in enumerate(ORDERS):
            spread("pair", colour, (LOW, every, at(d3, 2)), partner)
            spread("pair", colour, (HIGH, every, at(d3, 2)), partner)

    def gather_6():
        take("pair")

    def term(ref, colour, first, second, third, taps=None):
        iy, ix, iz = place(colour, first, second, third)
        taps = pl.ds(9 * colour, 9) if taps is None else taps
        if ref is partial:
            return (core, taps, iy, ix, iz)
        return (taps, iy, ix, iz)

    def pass_on(key, colour, where, dst, device):
        src = partial.at[term(partial, colour, *where)]
        copy = send(src, dst.at[term(dst, colour, *where)], device)
        waiting.setdefault(key, []).append(copy)

    def add(colour, where, *others):
        def one(tap, carry):
            tap = tap + 9 * colour
            mine = term(partial, colour, *where, taps=tap)
            total = partial[mine].astype(F32)
            for ref in others:
                total = total + ref[term(ref, colour, *where, taps=tap)].astype(F32)
            partial[mine] = total.astype(BF16)
            return carry

        lax.fori_loop(0, 9, one, 0)

    def reduce_pair(colour):
        taps = pl.ds(9 * colour, 9)
        copy = send(partial.at[1 - core, taps], from_partner.at[taps], partner)
        waiting.setdefault(f"p{colour}", []).append(copy)

    def reduce_phase(phase, part):
        plus, minus = (rx3p, rx3m) if phase == 3 else (rx2p, rx2m)
        for colour, order in enumerate(ORDERS):
            dim = order[phase - 1]

            def where(half, delta):
                if phase == 3:
                    return (half, every, at(dim, delta))
                return (half, at(dim, delta), own[order[2]])

            forward, backward = neighbour(dim, 1), neighbour(dim, -1)
            if part == 0:
                key = f"far{phase}{colour}"
                pass_on(key, colour, where(LOW, 2), plus, forward)
                pass_on(key, colour, where(HIGH, 2), minus, backward)
                key = f"near{phase}{colour}"
                pass_on(key, colour, where(HIGH, 1), plus, forward)
                pass_on(key, colour, where(LOW, -1), minus, backward)
            elif part == 1:
                take(f"far{phase}{colour}")
                key = f"near{phase}{colour}"
                add(colour, where(LOW, 1), plus)
                pass_on(key, colour, where(LOW, 1), plus, forward)
                add(colour, where(HIGH, -1), minus)
                pass_on(key, colour, where(HIGH, -1), minus, backward)
            else:
                take(f"near{phase}{colour}")
                add(colour, where(every, 0), plus, minus)

    def reduce_1():
        for colour in range(3):
            take(f"p{colour}")
            add(colour, (every, every, every), from_partner)
        reduce_phase(3, 0)

    def reduce_2():
        reduce_phase(3, 1)

    def reduce_3():
        reduce_phase(3, 2)
        reduce_phase(2, 0)

    def reduce_4():
        reduce_phase(2, 1)

    def reduce_5():
        reduce_phase(2, 2)
        for colour, (d1, d2, d3) in enumerate(ORDERS):
            for number, delta in enumerate((1, -1, 2)):
                src = partial.at[term(partial, colour, at(d1, delta), own[d2], own[d3])]
                dst = rx1.at[number, pl.ds(9 * colour, 9)]
                waiting.setdefault("r6", []).append(send(src, dst, neighbour(d1, delta)))

    def reduce_6():
        take("r6")
        for tap in range(27):
            total = partial[core, tap, y, x, zl].astype(F32)
            for number in range(3):
                total = total + rx1[number, tap].astype(F32)
            own_sum[tap] = total.astype(BF16)
        waiting["r7"] = [send(own_sum, other_sum, across)]

    def reduce_7(scale):
        take("r7")
        final_own[...] = (own_sum[...].astype(F32) + other_sum[...].astype(F32)) * scale
        waiting["r8"] = [send(final_own, final_other, partner)]
        grad_kernel[core] = final_own[...]

    def reduce_8():
        take("r8")
        grad_kernel[1 - core] = final_other[...]

    def shifted(values):
        rows = values.shape[0]
        w = lax.broadcasted_iota(jnp.int32, values.shape, 0) % 16
        before = jnp.where(w == 0, 0.0, pltpu.roll(values, 1, axis=0))
        after = jnp.where(w == 15, 0.0, pltpu.roll(values, rows - 1, axis=0))
        return before.astype(BF16), values.astype(BF16), after.astype(BF16)

    def put_hidden(values, d, h, count):
        for number, part in enumerate(shifted(values)):
            hidden3[number, d, pl.ds(h, count)] = part.reshape(count, 16, 512)

    def put_cot(values, d, h, count):
        for number, part in enumerate(shifted(values)):
            cot3[2 - number, d, pl.ds(h, count)] = part.reshape(count, 16, 256)

    def prepare_cot():
        for ref, width in ((cot3, 256), (hidden3, 512)):
            edge = jnp.zeros((3, 4, 16, width), BF16)
            ref[:, :, 0] = edge
            ref[:, :, 17] = edge

        def one(i, carry):
            d, h = i // 4, (i % 4) * 4
            values = cot[d, pl.ds(h, 4)].astype(F32).reshape(64, 256)
            put_cot(values, d + 1, h + 1, 4)
            return carry

        lax.fori_loop(0, 8, one, 0)

    def prepare_hidden():
        for i in range(4):
            d, h = i // 2, (i % 2) * 8
            values = silu(acts[d, pl.ds(h, 8)].astype(F32).reshape(128, 512))
            put_hidden(values, d + 1, h + 1, 8)
            hidden_t[:, 128 * i : 128 * i + 128] = values.T.astype(BF16)

    def fill_halo(number):
        take_halo(number)
        halo, put, width = (
            (halo_cot, put_cot, 256) if number == 0 else (halo_acts, put_hidden, 512)
        )
        for side, there in ((0, space > 0), (1, space < 3)):

            @pl.when(there)
            def _():
                def one(i, carry):
                    values = halo[side, pl.ds(i * 4, 4)].astype(F32).reshape(64, width)
                    put(silu(values) if number == 1 else values, 3 * side, i * 4 + 1, 4)
                    return carry

                lax.fori_loop(0, 4, one, 0)

            @pl.when(jnp.logical_not(there))
            def _():
                target = cot3 if number == 0 else hidden3
                target[:, 3 * side] = jnp.zeros((3, 18, 16, width), BF16)

    def cot_rows(colour, b, number):
        rows = cot3[number, pl.ds(2 - colour, 2), pl.ds(2 - b, 16)]
        return rows.reshape(512, 256)

    def kernel_term(colour, b):
        def one(number, carry):
            product = jnp.dot(
                hidden_t[...], cot_rows(colour, b, number), preferred_element_type=F32
            )
            tap = 9 * colour + 3 * b + number
            for half in range(2):
                part = product[:, 128 * half : 128 * half + 128]
                partial[half, tap] = part.reshape(4, 4, 4, 8, 128).astype(BF16)
            return carry

        lax.fori_loop(0, 3, one, 0)

    def tap_weight(tap):
        halves = [weights[half, tap].reshape(512, 128) for half in range(2)]
        return jnp.concatenate(halves, axis=1)

    def forward_and_back(colour, b, first):
        taps = [tap_weight(9 * colour + 3 * b + number) for number in range(3)]
        rows = [
            hidden3[number, pl.ds(colour, 2), pl.ds(b, 16)].reshape(512, 512)
            for number in range(3)
        ]
        product = jnp.dot(
            jnp.concatenate(rows, axis=1),
            jnp.concatenate(taps, axis=0),
            preferred_element_type=F32,
        )
        acc_out[...] = product if first else acc_out[...] + product
        grads = [cot_rows(colour, b, number) for number in range(3)]
        product = lax.dot_general(
            jnp.concatenate(grads, axis=1),
            jnp.concatenate(taps, axis=1),
            (((1,), (1,)), ((), ())),
            preferred_element_type=F32,
        )
        acc_back[...] = product if first else acc_back[...] + product

    gather_0()
    start_halo(0)
    start_halo(1)
    mine = pltpu.make_async_copy(shard.at[core], weights.at[core, :, y, x, zl], local_sem)
    mine.start()
    prepare_cot()
    prepare_hidden()
    mine.wait()
    gather_1()
    kernel_term(1, 0)
    kernel_term(1, 1)
    gather_2()
    kernel_term(1, 2)
    reduce_pair(1)
    gather_3()
    fill_halo(0)
    for b in range(3):
        kernel_term(0, b)
    reduce_pair(0)
    kernel_term(2, 0)
    gather_4()
    kernel_term(2, 1)
    kernel_term(2, 2)
    reduce_pair(2)
    reduce_1()
    gather_5()
    fill_halo(1)
    gather_6()
    forward_and_back(1, 0, True)
    forward_and_back(1, 1, False)
    reduce_2()
    forward_and_back(1, 2, False)
    forward_and_back(0, 0, False)
    reduce_3()
    forward_and_back(0, 1, False)
    reduce_4()
    forward_and_back(0, 2, False)
    reduce_5()
    forward_and_back(2, 0, False)
    reduce_6()
    forward_and_back(2, 1, False)
    forward_and_back(2, 2, False)
    reduce_7(1.0 / lax.axis_size("fsdp"))
    outputs[...] = acc_out[...].astype(BF16).reshape(outputs.shape)
    for i in range(8):
        d, h = i // 4, (i % 4) * 4
        values = acts[d, pl.ds(h, 4)].astype(F32).reshape(64, 512)
        squash = jax.nn.sigmoid(values)
        slope = squash * (1.0 + values * (1.0 - squash))
        total = acc_back[64 * i : 64 * i + 64] * slope
        grad_input[d, pl.ds(h, 4)] = total.astype(BF16).reshape(4, 16, 512)
    reduce_8()
    for copy in sent:
        copy.wait_send()
    end_halo(0)
    end_halo(1)


def body(acts, kernel, cotangent):
    shard = kernel.reshape(8, 27, 2, 128).transpose(2, 1, 0, 3)
    vmem = pl.BlockSpec(memory_space=pltpu.VMEM)
    whole = (27, 4, 4, 4, 8, 128)
    outputs, grad_input, grad_kernel = pl.pallas_call(
        step_kernel,
        out_shape=(
            jax.ShapeDtypeStruct((2, 16, 16, 256), BF16),
            jax.ShapeDtypeStruct((2, 16, 16, 512), BF16),
            jax.ShapeDtypeStruct((2, 27, 8, 128), F32),
        ),
        in_specs=[vmem] * 3,
        out_specs=(vmem,) * 3,
        scratch_shapes=[
            pltpu.VMEM((2, *whole), BF16),
            pltpu.VMEM((2, *whole), BF16),
            pltpu.VMEM(whole, BF16),
            pltpu.VMEM(whole, BF16),
            pltpu.VMEM(whole, BF16),
            pltpu.VMEM(whole, BF16),
            pltpu.VMEM(whole, BF16),
            pltpu.VMEM((3, 27, 8, 128), BF16),
            pltpu.VMEM((27, 8, 128), BF16),
            pltpu.VMEM((27, 8, 128), BF16),
            pltpu.VMEM((27, 8, 128), F32),
            pltpu.VMEM((27, 8, 128), F32),
            pltpu.VMEM((3, 4, 18, 16, 512), BF16),
            pltpu.VMEM((3, 4, 18, 16, 256), BF16),
            pltpu.VMEM((512, 512), BF16),
            pltpu.VMEM((2, 16, 16, 512), BF16),
            pltpu.VMEM((2, 16, 16, 256), BF16),
            pltpu.VMEM((512, 256), F32),
            pltpu.VMEM((512, 512), F32),
            pltpu.SemaphoreType.DMA((COPIES,)),
            pltpu.SemaphoreType.DMA((COPIES,)),
            pltpu.SemaphoreType.DMA,
        ],
        compiler_params=pltpu.CompilerParams(
            collective_id=0, has_side_effects=True, vmem_limit_bytes=66_000_000
        ),
        cost_estimate=pl.CostEstimate(
            flops=11_000_000_000, bytes_accessed=4_000_000, transcendentals=1_000_000
        ),
    )(acts[0], cotangent[0], shard)
    grad_kernel = grad_kernel.transpose(2, 1, 0, 3).reshape(8, 27, 256)
    return outputs[None], grad_input[None], grad_kernel


def solution(mesh):
    return jax.shard_map(
        body,
        mesh=mesh,
        in_specs=(
            P("fsdp", "space", None, None, None),
            P("fsdp", None, None),
            P("fsdp", "space", None, None, None),
        ),
        out_specs=(
            P("fsdp", "space", None, None, None),
            P("fsdp", "space", None, None, None),
            P("fsdp", None, None),
        ),
        check_vma=False,
    )
```

```python
import jax
import jax.numpy as jnp
from jax import lax
from jax.experimental import pallas as pl
from jax.experimental.pallas import tpu as pltpu
from jax.sharding import PartitionSpec as P

MESH = pl.DeviceIdType.MESH
F32 = jnp.float32
BF16 = jnp.bfloat16
ORDERS = (("z", "x", "y"), ("y", "z", "x"), ("x", "y", "z"))
LOW, HIGH = pl.ds(0, 2), pl.ds(2, 2)
COPIES = 128


def silu(v):
    return v * jax.nn.sigmoid(v)


def step_kernel(
    acts,
    cot,
    shard,
    outputs,
    grad_input,
    grad_kernel,
    weights,
    partial,
    from_partner,
    rx3p,
    rx3m,
    rx2p,
    rx2m,
    rx1,
    own_sum,
    other_sum,
    final_own,
    final_other,
    hidden3,
    cot3,
    hidden_t,
    halo_cot,
    edge_out,
    edge_in,
    acc_out,
    acc_back,
    send_sem,
    recv_sem,
    local_sem,
):
    space, fsdp = lax.axis_index("space"), lax.axis_index("fsdp")
    core, z_hi = space % 2, space // 2
    y, x, zl = fsdp // 16, (fsdp // 4) % 4, fsdp % 4
    z = z_hi * 4 + zl
    own = {"y": y, "x": x, "z": zl}

    def neighbour(dim, delta):
        if dim == "y":
            return (space, ((y + 4 + delta) % 4) * 16 + x * 4 + zl)
        if dim == "x":
            return (space, y * 16 + ((x + 4 + delta) % 4) * 4 + zl)
        there = (z + 8 + delta) % 8
        return ((there // 4) * 2 + core, y * 16 + x * 4 + there % 4)

    partner = (z_hi * 2 + 1 - core, fsdp)
    across = ((space + 2) % 4, fsdp)
    greeted = [neighbour(d, k) for d in ("y", "x") for k in (1, -1, 2)]
    greeted += [neighbour("z", k) for k in (1, -1, 2, -2)]
    greeted += [partner, across, (3 - space, fsdp)]

    barrier = pltpu.get_barrier_semaphore()
    for device in greeted:
        pl.semaphore_signal(barrier, inc=1, device_id=device, device_id_type=MESH)

    counter = [0]
    sent = []

    def remote(src, dst, device):
        number = counter[0]
        counter[0] += 1
        return pltpu.make_async_remote_copy(
            src_ref=src,
            dst_ref=dst,
            send_sem=send_sem.at[number],
            recv_sem=recv_sem.at[number],
            device_id=device,
            device_id_type=MESH,
        )

    def send(src, dst, device):
        copy = remote(src, dst, device)
        copy.start()
        sent.append(copy)
        return copy

    def at(dim, delta):
        return (own[dim] + 4 + delta) % 4

    def place(colour, first, second, third):
        d1, d2, d3 = ORDERS[colour]
        index = {d1: first, d2: second, d3: third}
        return index["y"], index["x"], index["z"]

    every = slice(None)

    lanes = pl.ds(pl.multiple_of(core * 128, 128), 128)
    other_lanes = pl.ds(pl.multiple_of((1 - core) * 128, 128), 128)

    def down_copy(src, dst):
        return remote(src, dst, (space - 1, fsdp))

    def up_copy(src, dst):
        return remote(src, dst, (space + 1, fsdp))

    def when_low(action):
        pl.when(space > 0)(action)

    def when_high(action):
        pl.when(space < 3)(action)

    cot_down = down_copy(cot.at[0], halo_cot.at[1])
    cot_up = up_copy(cot.at[1], halo_cot.at[0])
    edge_down = down_copy(edge_out.at[0], edge_in.at[1])
    edge_up = up_copy(edge_out.at[1], edge_in.at[0])

    def slot(colour, first, second, third):
        iy, ix, iz = place(colour, first, second, third)
        return weights.at[core, pl.ds(9 * colour, 9), iy, ix, iz]

    waiting = {}

    def spread(key, colour, where, device):
        piece = slot(colour, *where)
        waiting.setdefault(key, []).append(send(piece, piece, device))

    def take(key):
        for copy in waiting.pop(key):
            copy.wait_recv()

    def gather_0(colour):
        d1, d2, d3 = ORDERS[colour]
        here = slot(colour, own[d1], own[d2], own[d3])
        for delta in (1, -1, 2):
            copy = send(shard.at[pl.ds(9 * colour, 9), :, lanes], here, neighbour(d1, delta))
            waiting.setdefault(f"a1{colour}", []).append(copy)

    def gather_1(colour):
        d1, d2, d3 = ORDERS[colour]
        take(f"a1{colour}")
        for delta in (1, -1):
            spread(f"a2{colour}", colour, (every, own[d2], own[d3]), neighbour(d2, delta))

    def gather_2(colour):
        d1, d2, d3 = ORDERS[colour]
        take(f"a2{colour}")
        spread(f"a3{colour}", colour, (LOW, at(d2, -1), own[d3]), neighbour(d2, 1))
        spread(f"a3{colour}", colour, (HIGH, at(d2, 1), own[d3]), neighbour(d2, -1))

    def gather_3(colour):
        d1, d2, d3 = ORDERS[colour]
        take(f"a3{colour}")
        for delta in (1, -1):
            spread(f"a4{colour}", colour, (every, every, own[d3]), neighbour(d3, delta))
        spread(f"pair{colour}", colour, (every, every, own[d3]), partner)

    def gather_4(colour):
        d1, d2, d3 = ORDERS[colour]
        take(f"a4{colour}")
        spread(f"a5{colour}", colour, (LOW, every, at(d3, -1)), neighbour(d3, 1))
        spread(f"a5{colour}", colour, (HIGH, every, at(d3, 1)), neighbour(d3, -1))
        for delta in (1, -1):
            spread(f"pair{colour}", colour, (every, every, at(d3, delta)), partner)

    def gather_5(colour):
        d1, d2, d3 = ORDERS[colour]
        take(f"a5{colour}")
        spread(f"pair{colour}", colour, (LOW, every, at(d3, 2)), partner)
        spread(f"pair{colour}", colour, (HIGH, every, at(d3, 2)), partner)

    def gather_6(colour):
        take(f"pair{colour}")

    def term(ref, colour, first, second, third, taps=None):
        iy, ix, iz = place(colour, first, second, third)
        taps = pl.ds(9 * colour, 9) if taps is None else taps
        if ref is partial:
            return (core, taps, iy, ix, iz)
        return (taps, iy, ix, iz)

    def pass_on(key, colour, where, dst, device):
        src = partial.at[term(partial, colour, *where)]
        copy = send(src, dst.at[term(dst, colour, *where)], device)
        waiting.setdefault(key, []).append(copy)

    def add(colour, where, *others):
        def one(tap, carry):
            tap = tap + 9 * colour
            mine = term(partial, colour, *where, taps=tap)
            total = partial[mine].astype(F32)
            for ref in others:
                total = total + ref[term(ref, colour, *where, taps=tap)].astype(F32)
            partial[mine] = total.astype(BF16)
            return carry

        lax.fori_loop(0, 9, one, 0)

    def reduce_pair(key, tap, count):
        taps = pl.ds(tap, count)
        copy = send(partial.at[1 - core, taps], from_partner.at[taps], partner)
        waiting.setdefault(key, []).append(copy)

    def reduce_phase(phase, part, colour):
        plus, minus = (rx3p, rx3m) if phase == 3 else (rx2p, rx2m)
        order = ORDERS[colour]
        dim = order[phase - 1]
        forward, backward = neighbour(dim, 1), neighbour(dim, -1)
        far, near = f"far{phase}{colour}", f"near{phase}{colour}"

        def where(half, delta):
            if phase == 3:
                return (half, every, at(dim, delta))
            return (half, at(dim, delta), own[order[2]])

        if part == 0:
            pass_on(far, colour, where(LOW, 2), plus, forward)
            pass_on(far, colour, where(HIGH, 2), minus, backward)
            pass_on(near, colour, where(HIGH, 1), plus, forward)
            pass_on(near, colour, where(LOW, -1), minus, backward)
        elif part == 1:
            take(far)
            add(colour, where(LOW, 1), plus)
            pass_on(near, colour, where(LOW, 1), plus, forward)
            add(colour, where(HIGH, -1), minus)
            pass_on(near, colour, where(HIGH, -1), minus, backward)
        else:
            take(near)
            add(colour, where(every, 0), plus, minus)

    def reduce_1(colour):
        for key in ("p1",) if colour == 1 else ("p first", "p second"):
            if key in waiting:
                take(key)
        add(colour, (every, every, every), from_partner)
        reduce_phase(3, 0, colour)

    def reduce_2(colour):
        reduce_phase(3, 1, colour)

    def reduce_3(colour):
        reduce_phase(3, 2, colour)
        reduce_phase(2, 0, colour)

    def reduce_4(colour):
        reduce_phase(2, 1, colour)

    def reduce_5(colour):
        reduce_phase(2, 2, colour)
        d1, d2, d3 = ORDERS[colour]
        for number, delta in enumerate((1, -1, 2)):
            src = partial.at[term(partial, colour, at(d1, delta), own[d2], own[d3])]
            dst = rx1.at[number, pl.ds(9 * colour, 9)]
            copy = send(src, dst, neighbour(d1, delta))
            waiting.setdefault(f"r6{colour}", []).append(copy)

    def reduce_6(colour):
        take(f"r6{colour}")
        for tap in range(9 * colour, 9 * colour + 9):
            total = partial[core, tap, y, x, zl].astype(F32)
            for number in range(3):
                total = total + rx1[number, tap].astype(F32)
            own_sum[tap] = total.astype(BF16)
        taps = pl.ds(9 * colour, 9)
        waiting[f"r7{colour}"] = [send(own_sum.at[taps], other_sum.at[taps], across)]

    def reduce_7(scale):
        for colour in range(3):
            take(f"r7{colour}")
        final_own[...] = (own_sum[...].astype(F32) + other_sum[...].astype(F32)) * scale
        waiting["r8"] = [send(final_own, final_other, partner)]
        grad_kernel[:, :, lanes] = final_own[...]

    def reduce_8():
        take("r8")
        grad_kernel[:, :, other_lanes] = final_other[...]

    def shifted(values):
        rows = values.shape[0]
        w = lax.broadcasted_iota(jnp.int32, values.shape, 0) % 16
        before = jnp.where(w == 0, 0.0, pltpu.roll(values, 1, axis=0))
        after = jnp.where(w == 15, 0.0, pltpu.roll(values, rows - 1, axis=0))
        return before.astype(BF16), values.astype(BF16), after.astype(BF16)

    def put_hidden(values, d, h, count):
        for number, part in enumerate(shifted(values)):
            hidden3[number, d, pl.ds(h, count)] = part.reshape(count, 16, 512)

    def put_cot(values, d, h, count):
        for number, part in enumerate(shifted(values)):
            cot3[2 - number, d, pl.ds(h, count)] = part.reshape(count, 16, 256)

    def prepare_cot():
        for ref, width in ((cot3, 256), (hidden3, 512)):
            edge = jnp.zeros((3, ref.shape[1], 16, width), BF16)
            ref[:, :, 0] = edge
            ref[:, :, 17] = edge

        def one(i, carry):
            d, h = i // 4, (i % 4) * 4
            values = cot[d, pl.ds(h, 4)].astype(F32).reshape(64, 256)
            put_cot(values, d + 1, h + 1, 4)
            return carry

        lax.fori_loop(0, 8, one, 0)

    def prepare_hidden():
        for i in range(4):
            d, h = i // 2, (i % 2) * 8
            values = silu(acts[d, pl.ds(h, 8)].astype(F32).reshape(128, 512))
            put_hidden(values, d, h + 1, 8)
            hidden_t[:, 128 * i : 128 * i + 128] = values.T.astype(BF16)

    def fill_halo(side):
        (cot_down if side else cot_up).wait_recv()

        def one(i, carry):
            values = halo_cot[side, pl.ds(i * 4, 4)].astype(F32).reshape(64, 256)
            put_cot(values, 3 * side, i * 4 + 1, 4)
            return carry

        lax.fori_loop(0, 4, one, 0)

    def fill_near():
        for side in range(2):
            pl.when(core == 1 - side)(lambda: fill_halo(side))

    def fill_far():
        pl.when(space == 1)(lambda: fill_halo(1))
        pl.when(space == 2)(lambda: fill_halo(0))

    def no_halo():
        for side in range(2):

            @pl.when(space == 3 * side)
            def _():
                cot3[:, 3 * side] = jnp.zeros((3, 18, 16, 256), BF16)
                edge_in[side] = jnp.zeros((256, 256), BF16)

    def cot_rows(colour, b, number):
        rows = cot3[number, pl.ds(2 - colour, 2), pl.ds(2 - b, 16)]
        return rows.reshape(512, 256)

    def kernel_term(colour, b):
        rows = [cot_rows(colour, b, number) for number in range(3)]
        product = jnp.dot(
            hidden_t[...], jnp.concatenate(rows, axis=1), preferred_element_type=F32
        )
        for number in range(3):
            for half in range(2):
                start = 256 * number + 128 * half
                part = product[:, start : start + 128].reshape(4, 4, 4, 8, 128)
                partial[half, 9 * colour + 3 * b + number] = part.astype(BF16)

    def tap_weight(tap):
        halves = [weights[half, tap].reshape(512, 128) for half in range(2)]
        return jnp.concatenate(halves, axis=1)

    def forward_and_back(colour, b):
        taps = [tap_weight(9 * colour + 3 * b + number) for number in range(3)]
        rows = [hidden3[number, :, pl.ds(b, 16)].reshape(512, 512) for number in range(3)]
        product = jnp.dot(
            jnp.concatenate(rows, axis=1),
            jnp.concatenate(taps, axis=0),
            preferred_element_type=F32,
        )
        acc_out[colour] = product if b == 0 else acc_out[colour] + product
        grads = [cot_rows(colour, b, number) for number in range(3)]
        product = lax.dot_general(
            jnp.concatenate(grads, axis=1),
            jnp.concatenate(taps, axis=1),
            (((1,), (1,)), ((), ())),
            preferred_element_type=F32,
        )
        acc_back[...] = product if colour == 0 and b == 0 else acc_back[...] + product

    def send_edge_up():
        edge_out[1] = acc_out[0, 256:].astype(BF16)
        when_high(edge_up.start)

    def send_edge_down():
        edge_out[0] = acc_out[2, :256].astype(BF16)
        when_low(edge_down.start)

    def write_outputs():
        when_low(edge_up.wait_recv)
        total = acc_out[1, :256] + acc_out[2, 256:] + edge_in[0].astype(F32)
        outputs[0] = total.astype(BF16).reshape(16, 16, 256)
        when_high(edge_down.wait_recv)
        total = acc_out[1, 256:] + acc_out[0, :256] + edge_in[1].astype(F32)
        outputs[1] = total.astype(BF16).reshape(16, 16, 256)

    def write_grad_input():
        for i in range(8):
            d, h = i // 4, (i % 4) * 4
            values = acts[d, pl.ds(h, 4)].astype(F32).reshape(64, 512)
            squash = jax.nn.sigmoid(values)
            slope = squash * (1.0 + values * (1.0 - squash))
            total = acc_back[64 * i : 64 * i + 64] * slope
            grad_input[d, pl.ds(h, 4)] = total.astype(BF16).reshape(4, 16, 512)

    def finish():
        for copy in sent:
            copy.wait_send()

        @when_low
        def _():
            cot_down.wait_send()
            edge_down.wait_send()

        @when_high
        def _():
            cot_up.wait_send()
            edge_up.wait_send()

    first, second = 2 - 2 * z_hi, 2 * z_hi

    def near_term(b):
        kernel_term(first, b)
        reduce_pair("p first", 9 * first + 3 * b, 3)

    def far_term(b):
        kernel_term(second, b)
        reduce_pair("p second", 9 * second + 3 * b, 3)

    prepare_cot()
    prepare_hidden()
    no_halo()
    kernel_term(1, 0)
    kernel_term(1, 1)
    kernel_term(1, 2)
    pl.semaphore_wait(barrier, len(greeted))
    gather_0(0)
    gather_0(1)
    gather_0(2)
    when_low(cot_down.start)
    when_high(cot_up.start)
    mine = pltpu.make_async_copy(
        shard.at[:, :, lanes], weights.at[core, :, y, x, zl], local_sem
    )
    mine.start()
    reduce_pair("p1", 9, 9)
    fill_near()
    near_term(0)
    near_term(1)
    near_term(2)
    mine.wait()
    gather_1(1)
    gather_1(2)
    gather_1(0)
    fill_far()
    far_term(0)
    far_term(1)
    gather_2(2)
    gather_2(1)
    gather_2(0)
    far_term(2)
    reduce_1(1)
    reduce_1(0)
    reduce_1(2)
    gather_3(2)
    gather_3(1)
    gather_3(0)
    reduce_2(1)
    reduce_2(0)
    reduce_2(2)
    gather_4(1)
    gather_4(0)
    gather_4(2)
    reduce_3(1)
    reduce_3(0)
    reduce_3(2)
    reduce_4(1)
    gather_5(1)
    gather_5(0)
    gather_5(2)
    reduce_4(0)
    reduce_4(2)
    gather_6(0)
    forward_and_back(0, 0)
    reduce_5(1)
    forward_and_back(0, 1)
    reduce_5(0)
    forward_and_back(0, 2)
    send_edge_up()
    reduce_5(2)
    gather_6(2)
    forward_and_back(2, 0)
    reduce_6(1)
    forward_and_back(2, 1)
    reduce_6(0)
    forward_and_back(2, 2)
    send_edge_down()
    reduce_6(2)
    gather_6(1)
    forward_and_back(1, 0)
    forward_and_back(1, 1)
    forward_and_back(1, 2)
    write_grad_input()
    reduce_7(1.0 / lax.axis_size("fsdp"))
    write_outputs()
    reduce_8()
    finish()


def write_kernel(outputs, grad_input, grad_kernel, outputs_to, grad_input_to, grad_kernel_to):
    outputs_to[...] = outputs[...]
    grad_input_to[...] = grad_input[...]
    grad_kernel_to[...] = grad_kernel[...]


def body(acts, kernel, cotangent):
    vmem = pl.BlockSpec(memory_space=pltpu.VMEM)
    whole = (27, 4, 4, 4, 8, 128)
    results = (
        jax.ShapeDtypeStruct((2, 16, 16, 256), BF16),
        jax.ShapeDtypeStruct((2, 16, 16, 512), BF16),
        jax.ShapeDtypeStruct((27, 8, 256), F32),
    )
    computed = pl.pallas_call(
        step_kernel,
        out_shape=results,
        in_specs=[vmem] * 3,
        out_specs=(vmem,) * 3,
        scratch_shapes=[
            pltpu.VMEM((2, *whole), BF16),
            pltpu.VMEM((2, *whole), BF16),
            pltpu.VMEM(whole, BF16),
            pltpu.VMEM(whole, BF16),
            pltpu.VMEM(whole, BF16),
            pltpu.VMEM(whole, BF16),
            pltpu.VMEM(whole, BF16),
            pltpu.VMEM((3, 27, 8, 128), BF16),
            pltpu.VMEM((27, 8, 128), BF16),
            pltpu.VMEM((27, 8, 128), BF16),
            pltpu.VMEM((27, 8, 128), F32),
            pltpu.VMEM((27, 8, 128), F32),
            pltpu.VMEM((3, 2, 18, 16, 512), BF16),
            pltpu.VMEM((3, 4, 18, 16, 256), BF16),
            pltpu.VMEM((512, 512), BF16),
            pltpu.VMEM((2, 16, 16, 256), BF16),
            pltpu.VMEM((2, 256, 256), BF16),
            pltpu.VMEM((2, 256, 256), BF16),
            pltpu.VMEM((3, 512, 256), F32),
            pltpu.VMEM((512, 512), F32),
            pltpu.SemaphoreType.DMA((COPIES,)),
            pltpu.SemaphoreType.DMA((COPIES,)),
            pltpu.SemaphoreType.DMA,
        ],
        compiler_params=pltpu.CompilerParams(
            collective_id=0, has_side_effects=True, vmem_limit_bytes=54_000_000
        ),
        cost_estimate=pl.CostEstimate(
            flops=11_000_000_000, bytes_accessed=4_000_000, transcendentals=1_000_000
        ),
    )(acts[0], cotangent[0], kernel.transpose(1, 0, 2))
    outputs, grad_input, grad_kernel = pl.pallas_call(
        write_kernel,
        out_shape=results,
        in_specs=[vmem] * 3,
        out_specs=(vmem,) * 3,
        compiler_params=pltpu.CompilerParams(vmem_limit_bytes=8_000_000),
    )(*computed)
    return outputs[None], grad_input[None], grad_kernel.transpose(1, 0, 2)


def solution(mesh):
    return jax.shard_map(
        body,
        mesh=mesh,
        in_specs=(
            P("fsdp", "space", None, None, None),
            P("fsdp", None, None),
            P("fsdp", "space", None, None, None),
        ),
        out_specs=(
            P("fsdp", "space", None, None, None),
            P("fsdp", "space", None, None, None),
            P("fsdp", None, None),
        ),
        check_vma=False,
    )
```

```python
import jax
import jax.numpy as jnp
from jax import lax
from jax.experimental import pallas as pl
from jax.experimental.pallas import tpu as pltpu
from jax.sharding import PartitionSpec as P

MESH = pl.DeviceIdType.MESH
F32 = jnp.float32
BF16 = jnp.bfloat16
ORDERS = (("z", "x", "y"), ("y", "z", "x"), ("x", "y", "z"))
LOW, HIGH = pl.ds(0, 2), pl.ds(2, 2)
COPIES = 128


def silu(v):
    return v * jax.nn.sigmoid(v)


def step_kernel(
    acts_in,
    cot_in,
    shard_in,
    outputs,
    grad_input,
    grad_kernel,
    weights,
    partial,
    from_partner,
    rx3p,
    rx3m,
    rx2p,
    rx2m,
    rx1,
    own_sum,
    other_sum,
    final_own,
    final_other,
    hidden3,
    cot3,
    hidden_t,
    halo_cot,
    edge_out,
    edge_in,
    acc_edge,
    acc_mid,
    acc_back,
    acts,
    cot,
    shard,
    send_sem,
    recv_sem,
    local_sem,
):
    space, fsdp = lax.axis_index("space"), lax.axis_index("fsdp")
    core, z_hi = space % 2, space // 2
    y, x, zl = fsdp // 16, (fsdp // 4) % 4, fsdp % 4
    z = z_hi * 4 + zl
    own = {"y": y, "x": x, "z": zl}

    def neighbour(dim, delta):
        if dim == "y":
            return (space, ((y + 4 + delta) % 4) * 16 + x * 4 + zl)
        if dim == "x":
            return (space, y * 16 + ((x + 4 + delta) % 4) * 4 + zl)
        there = (z + 8 + delta) % 8
        return ((there // 4) * 2 + core, y * 16 + x * 4 + there % 4)

    partner = (z_hi * 2 + 1 - core, fsdp)
    across = ((space + 2) % 4, fsdp)
    greeted = [neighbour(d, k) for d in ("y", "x") for k in (1, -1, 2)]
    greeted += [neighbour("z", k) for k in (1, -1, 2, -2)]
    greeted += [partner, across, (3 - space, fsdp)]

    shard_copy = pltpu.make_async_copy(shard_in, shard, local_sem.at[1])
    cot_copy = pltpu.make_async_copy(cot_in, cot, local_sem.at[2])
    acts_copy = pltpu.make_async_copy(acts_in, acts, local_sem.at[3])
    shard_copy.start()
    cot_copy.start()
    acts_copy.start()

    barrier = pltpu.get_barrier_semaphore()
    for device in greeted:
        pl.semaphore_signal(barrier, inc=1, device_id=device, device_id_type=MESH)

    counter = [0]
    sent = []

    def remote(src, dst, device):
        number = counter[0]
        counter[0] += 1
        return pltpu.make_async_remote_copy(
            src_ref=src,
            dst_ref=dst,
            send_sem=send_sem.at[number],
            recv_sem=recv_sem.at[number],
            device_id=device,
            device_id_type=MESH,
        )

    def send(src, dst, device):
        copy = remote(src, dst, device)
        copy.start()
        sent.append(copy)
        return copy

    def at(dim, delta):
        return (own[dim] + 4 + delta) % 4

    def place(colour, first, second, third):
        d1, d2, d3 = ORDERS[colour]
        index = {d1: first, d2: second, d3: third}
        return index["y"], index["x"], index["z"]

    every = slice(None)

    lanes = pl.ds(pl.multiple_of(core * 128, 128), 128)
    other_lanes = pl.ds(pl.multiple_of((1 - core) * 128, 128), 128)

    def down_copy(src, dst):
        return remote(src, dst, (space - 1, fsdp))

    def up_copy(src, dst):
        return remote(src, dst, (space + 1, fsdp))

    def when_low(action):
        pl.when(space > 0)(action)

    def when_high(action):
        pl.when(space < 3)(action)

    cot_down = down_copy(cot.at[0], halo_cot.at[1])
    cot_up = up_copy(cot.at[1], halo_cot.at[0])
    edge_down = down_copy(edge_out.at[0], edge_in.at[1])
    edge_up = up_copy(edge_out.at[1], edge_in.at[0])

    def slot(colour, first, second, third):
        iy, ix, iz = place(colour, first, second, third)
        return weights.at[core, pl.ds(9 * colour, 9), iy, ix, iz]

    waiting = {}

    def spread(key, colour, where, device):
        piece = slot(colour, *where)
        waiting.setdefault(key, []).append(send(piece, piece, device))

    def take(key):
        for copy in waiting.pop(key):
            copy.wait_recv()

    def gather_0(colour):
        d1, d2, d3 = ORDERS[colour]
        here = slot(colour, own[d1], own[d2], own[d3])
        for delta in (1, -1, 2):
            copy = send(shard.at[pl.ds(9 * colour, 9), :, lanes], here, neighbour(d1, delta))
            waiting.setdefault(f"a1{colour}", []).append(copy)

    def gather_1(colour):
        d1, d2, d3 = ORDERS[colour]
        take(f"a1{colour}")
        for delta in (1, -1):
            spread(f"a2{colour}", colour, (every, own[d2], own[d3]), neighbour(d2, delta))

    def gather_2(colour):
        d1, d2, d3 = ORDERS[colour]
        take(f"a2{colour}")
        spread(f"a3{colour}", colour, (LOW, at(d2, -1), own[d3]), neighbour(d2, 1))
        spread(f"a3{colour}", colour, (HIGH, at(d2, 1), own[d3]), neighbour(d2, -1))

    def gather_3(colour):
        d1, d2, d3 = ORDERS[colour]
        take(f"a3{colour}")
        spread(f"a4{colour}", colour, (LOW, every, own[d3]), neighbour(d3, 1))
        spread(f"a4{colour}", colour, (HIGH, every, own[d3]), neighbour(d3, -1))
        spread(f"pair{colour}", colour, (every, every, own[d3]), partner)

    def gather_3b(colour):
        d1, d2, d3 = ORDERS[colour]
        spread(f"a5{colour}", colour, (HIGH, every, own[d3]), neighbour(d3, 1))
        spread(f"a5{colour}", colour, (LOW, every, own[d3]), neighbour(d3, -1))

    def gather_4(colour):
        d1, d2, d3 = ORDERS[colour]
        take(f"a4{colour}")
        spread(f"a5{colour}", colour, (LOW, every, at(d3, -1)), neighbour(d3, 1))
        spread(f"a5{colour}", colour, (HIGH, every, at(d3, 1)), neighbour(d3, -1))
        spread(f"pair{colour}", colour, (LOW, every, at(d3, -1)), partner)
        spread(f"pair{colour}", colour, (HIGH, every, at(d3, 1)), partner)

    def gather_5(colour):
        d1, d2, d3 = ORDERS[colour]
        take(f"a5{colour}")
        spread(f"pair{colour}", colour, (HIGH, every, at(d3, -1)), partner)
        spread(f"pair{colour}", colour, (LOW, every, at(d3, 1)), partner)
        spread(f"pair{colour}", colour, (every, every, at(d3, 2)), partner)

    def gather_6(colour):
        take(f"pair{colour}")

    def term(ref, colour, first, second, third, taps=None):
        iy, ix, iz = place(colour, first, second, third)
        taps = pl.ds(9 * colour, 9) if taps is None else taps
        if ref is partial:
            return (core, taps, iy, ix, iz)
        return (taps, iy, ix, iz)

    def pass_on(key, colour, where, dst, device):
        src = partial.at[term(partial, colour, *where)]
        copy = send(src, dst.at[term(dst, colour, *where)], device)
        waiting.setdefault(key, []).append(copy)

    def add(colour, where, *others):
        def one(tap, carry):
            tap = tap + 9 * colour
            mine = term(partial, colour, *where, taps=tap)
            total = partial[mine].astype(F32)
            for ref in others:
                total = total + ref[term(ref, colour, *where, taps=tap)].astype(F32)
            partial[mine] = total.astype(BF16)
            return carry

        lax.fori_loop(0, 9, one, 0)

    def reduce_pair(key, tap, count):
        taps = pl.ds(tap, count)
        copy = send(partial.at[1 - core, taps], from_partner.at[taps], partner)
        waiting.setdefault(key, []).append(copy)

    def reduce_phase(phase, part, colour):
        plus, minus = (rx3p, rx3m) if phase == 3 else (rx2p, rx2m)
        order = ORDERS[colour]
        dim = order[phase - 1]
        forward, backward = neighbour(dim, 1), neighbour(dim, -1)
        far, near = f"far{phase}{colour}", f"near{phase}{colour}"

        def where(half, delta):
            if phase == 3:
                return (half, every, at(dim, delta))
            return (half, at(dim, delta), own[order[2]])

        if part == "far":
            pass_on(far, colour, where(LOW, 2), plus, forward)
            pass_on(far, colour, where(HIGH, 2), minus, backward)
        elif part == "near":
            pass_on(near, colour, where(HIGH, 1), plus, forward)
            pass_on(near, colour, where(LOW, -1), minus, backward)
        elif part == 1:
            take(far)
            add(colour, where(LOW, 1), plus)
            pass_on(near, colour, where(LOW, 1), plus, forward)
            add(colour, where(HIGH, -1), minus)
            pass_on(near, colour, where(HIGH, -1), minus, backward)
        else:
            take(near)
            add(colour, where(every, 0), plus, minus)

    def reduce_1(colour):
        for key in ("p1",) if colour == 1 else ("p first", "p second"):
            if key in waiting:
                take(key)
        add(colour, (every, every, every), from_partner)
        reduce_phase(3, "far", colour)

    def reduce_1b(colour):
        reduce_phase(3, "near", colour)

    def reduce_2(colour):
        reduce_phase(3, 1, colour)

    def reduce_3(colour):
        reduce_phase(3, 2, colour)
        reduce_phase(2, "far", colour)
        reduce_phase(2, "near", colour)

    def reduce_4(colour):
        reduce_phase(2, 1, colour)

    def reduce_5(colour):
        reduce_phase(2, 2, colour)
        d1, d2, d3 = ORDERS[colour]
        for number, delta in enumerate((1, -1, 2)):
            src = partial.at[term(partial, colour, at(d1, delta), own[d2], own[d3])]
            dst = rx1.at[number, pl.ds(9 * colour, 9)]
            copy = send(src, dst, neighbour(d1, delta))
            waiting.setdefault(f"r6{colour}", []).append(copy)

    def reduce_6(colour):
        take(f"r6{colour}")
        for tap in range(9 * colour, 9 * colour + 9):
            total = partial[core, tap, y, x, zl].astype(F32)
            for number in range(3):
                total = total + rx1[number, tap].astype(F32)
            own_sum[tap] = total.astype(BF16)
        taps = pl.ds(9 * colour, 9)
        waiting[f"r7{colour}"] = [send(own_sum.at[taps], other_sum.at[taps], across)]

    def reduce_7(scale):
        for colour in range(3):
            take(f"r7{colour}")
        final_own[...] = (own_sum[...].astype(F32) + other_sum[...].astype(F32)) * scale
        waiting["r8"] = [send(final_own, final_other, partner)]
        grad_kernel[:, :, lanes] = final_own[...]

    def reduce_8():
        take("r8")
        grad_kernel[:, :, other_lanes] = final_other[...]

    def shifted(values):
        rows = values.shape[0]
        w = lax.broadcasted_iota(jnp.int32, values.shape, 0) % 16
        before = jnp.where(w == 0, 0.0, pltpu.roll(values, 1, axis=0))
        after = jnp.where(w == 15, 0.0, pltpu.roll(values, rows - 1, axis=0))
        return before.astype(BF16), values.astype(BF16), after.astype(BF16)

    def put_hidden(values, d, h, count):
        for number, part in enumerate(shifted(values)):
            hidden3[number, d, pl.ds(h, count)] = part.reshape(count, 16, 512)

    def put_cot(values, d, h, count):
        for number, part in enumerate(shifted(values)):
            cot3[2 - number, d, pl.ds(h, count)] = part.reshape(count, 16, 256)

    def prepare_cot():
        for ref, width in ((cot3, 256), (hidden3, 512)):
            edge = jnp.zeros((3, ref.shape[1], 16, width), BF16)
            ref[:, :, 0] = edge
            ref[:, :, 17] = edge

        def one(i, carry):
            d, h = i // 4, (i % 4) * 4
            values = cot[d, pl.ds(h, 4)].astype(F32).reshape(64, 256)
            put_cot(values, d + 1, h + 1, 4)
            return carry

        lax.fori_loop(0, 8, one, 0)

    def prepare_hidden():
        for i in range(4):
            d, h = i // 2, (i % 2) * 8
            values = silu(acts[d, pl.ds(h, 8)].astype(F32).reshape(128, 512))
            put_hidden(values, d, h + 1, 8)
            hidden_t[:, 128 * i : 128 * i + 128] = values.T.astype(BF16)

    def fill_halo(side):
        (cot_down if side else cot_up).wait_recv()

        def one(i, carry):
            values = halo_cot[side, pl.ds(i * 4, 4)].astype(F32).reshape(64, 256)
            put_cot(values, 3 * side, i * 4 + 1, 4)
            return carry

        lax.fori_loop(0, 4, one, 0)

    def fill_near():
        for side in range(2):
            pl.when(core == 1 - side)(lambda: fill_halo(side))

    def fill_far():
        pl.when(space == 1)(lambda: fill_halo(1))
        pl.when(space == 2)(lambda: fill_halo(0))

    def no_halo():
        for side in range(2):

            @pl.when(space == 3 * side)
            def _():
                cot3[:, 3 * side] = jnp.zeros((3, 18, 16, 256), BF16)
                edge_in[side] = jnp.zeros((256, 256), BF16)

    def cot_rows(colour, b, number):
        rows = cot3[number, pl.ds(2 - colour, 2), pl.ds(2 - b, 16)]
        return rows.reshape(512, 256)

    def kernel_term(colour, b):
        rows = [cot_rows(colour, b, number) for number in range(3)]
        product = jnp.dot(
            hidden_t[...], jnp.concatenate(rows, axis=1), preferred_element_type=F32
        )
        for number in range(3):
            for half in range(2):
                start = 256 * number + 128 * half
                part = product[:, start : start + 128].reshape(4, 4, 4, 8, 128)
                partial[half, 9 * colour + 3 * b + number] = part.astype(BF16)

    def tap_weight(tap):
        halves = [weights[half, tap].reshape(512, 128) for half in range(2)]
        return jnp.concatenate(halves, axis=1)

    def three_taps(colour, b):
        return [tap_weight(9 * colour + 3 * b + number) for number in range(3)]

    def hidden_rows(b):
        rows = [hidden3[number, :, pl.ds(b, 16)].reshape(512, 512) for number in range(3)]
        return jnp.concatenate(rows, axis=1)

    def back_product(colours, b, taps):
        grads = [cot_rows(colour, b, number) for colour in colours for number in range(3)]
        return lax.dot_general(
            jnp.concatenate(grads, axis=1),
            jnp.concatenate(taps, axis=1),
            (((1,), (1,)), ((), ())),
            preferred_element_type=F32,
        )

    def forward_edges(b):
        below, above = three_taps(0, b), three_taps(2, b)
        both = [jnp.concatenate(pair, axis=1) for pair in zip(below, above)]
        product = jnp.dot(
            hidden_rows(b), jnp.concatenate(both, axis=0), preferred_element_type=F32
        )
        acc_edge[...] = product if b == 0 else acc_edge[...] + product

    def back_edges(b):
        product = back_product((0, 2), b, three_taps(0, b) + three_taps(2, b))
        acc_back[...] = product if b == 0 else acc_back[...] + product

    def forward_and_back(b):
        taps = three_taps(1, b)
        product = jnp.dot(
            hidden_rows(b), jnp.concatenate(taps, axis=0), preferred_element_type=F32
        )
        acc_mid[...] = product if b == 0 else acc_mid[...] + product
        acc_back[...] = acc_back[...] + back_product((1,), b, taps)

    def send_edges():
        edge_out[1] = acc_edge[256:, :256].astype(BF16)
        when_high(edge_up.start)
        edge_out[0] = acc_edge[:256, 256:].astype(BF16)
        when_low(edge_down.start)

    def write_outputs():
        when_low(edge_up.wait_recv)
        total = acc_mid[:256] + acc_edge[256:, 256:] + edge_in[0].astype(F32)
        outputs[0] = total.astype(BF16).reshape(16, 16, 256)
        when_high(edge_down.wait_recv)
        total = acc_mid[256:] + acc_edge[:256, :256] + edge_in[1].astype(F32)
        outputs[1] = total.astype(BF16).reshape(16, 16, 256)

    def write_grad_input():
        for i in range(8):
            d, h = i // 4, (i % 4) * 4
            values = acts[d, pl.ds(h, 4)].astype(F32).reshape(64, 512)
            squash = jax.nn.sigmoid(values)
            slope = squash * (1.0 + values * (1.0 - squash))
            total = acc_back[64 * i : 64 * i + 64] * slope
            grad_input[d, pl.ds(h, 4)] = total.astype(BF16).reshape(4, 16, 512)

    def finish():
        for copy in sent:
            copy.wait_send()

        @when_low
        def _():
            cot_down.wait_send()
            edge_down.wait_send()

        @when_high
        def _():
            cot_up.wait_send()
            edge_up.wait_send()

    first, second = 2 - 2 * z_hi, 2 * z_hi

    def near_term(b):
        kernel_term(first, b)
        reduce_pair("p first", 9 * first + 3 * b, 3)

    def far_term(b):
        kernel_term(second, b)
        reduce_pair("p second", 9 * second + 3 * b, 3)

    pl.semaphore_wait(barrier, len(greeted))
    shard_copy.wait()
    gather_0(0)
    gather_0(1)
    gather_0(2)
    cot_copy.wait()
    when_low(cot_down.start)
    when_high(cot_up.start)
    mine = pltpu.make_async_copy(
        shard.at[:, :, lanes], weights.at[core, :, y, x, zl], local_sem.at[0]
    )
    mine.start()
    prepare_cot()
    acts_copy.wait()
    prepare_hidden()
    no_halo()
    kernel_term(1, 0)
    kernel_term(1, 1)
    kernel_term(1, 2)
    reduce_pair("p1", 9, 9)
    fill_near()
    near_term(0)
    near_term(1)
    mine.wait()
    gather_1(1)
    gather_1(2)
    gather_1(0)
    near_term(2)
    fill_far()
    far_term(0)
    far_term(1)
    far_term(2)
    reduce_1(1)
    reduce_1(0)
    reduce_1(2)
    gather_2(2)
    gather_2(1)
    gather_2(0)
    reduce_1b(1)
    reduce_1b(0)
    reduce_1b(2)
    reduce_2(1)
    reduce_2(0)
    reduce_2(2)
    gather_3(2)
    gather_3(1)
    gather_3(0)
    reduce_3(1)
    reduce_3(0)
    reduce_3(2)
    gather_3b(2)
    gather_3b(1)
    gather_3b(0)
    gather_4(2)
    gather_4(1)
    gather_4(0)
    reduce_4(1)
    reduce_4(0)
    reduce_4(2)
    reduce_5(1)
    reduce_5(0)
    reduce_5(2)
    gather_5(2)
    gather_5(0)
    gather_5(1)
    gather_6(2)
    gather_6(0)
    forward_edges(0)
    forward_edges(1)
    forward_edges(2)
    send_edges()
    reduce_6(1)
    reduce_6(0)
    reduce_6(2)
    back_edges(0)
    back_edges(1)
    back_edges(2)
    gather_6(1)
    forward_and_back(0)
    forward_and_back(1)
    forward_and_back(2)
    write_grad_input()
    reduce_7(1.0 / lax.axis_size("fsdp"))
    write_outputs()
    reduce_8()
    finish()


def write_kernel(outputs, grad_input, grad_kernel, outputs_to, grad_input_to, grad_kernel_to):
    outputs_to[...] = outputs[...]
    grad_input_to[...] = grad_input[...]
    grad_kernel_to[...] = grad_kernel[...]


def in_hbm(value):
    return pltpu.with_memory_space_constraint(value, pltpu.HBM)


def body(acts, kernel, cotangent):
    vmem = pl.BlockSpec(memory_space=pltpu.VMEM)
    whole = (27, 4, 4, 4, 8, 128)
    results = (
        jax.ShapeDtypeStruct((2, 16, 16, 256), BF16),
        jax.ShapeDtypeStruct((2, 16, 16, 512), BF16),
        jax.ShapeDtypeStruct((27, 8, 256), F32),
    )
    computed = pl.pallas_call(
        step_kernel,
        out_shape=results,
        in_specs=[pl.BlockSpec(memory_space=pltpu.HBM)] * 3,
        out_specs=(vmem,) * 3,
        scratch_shapes=[
            pltpu.VMEM((2, *whole), BF16),
            pltpu.VMEM((2, *whole), BF16),
            pltpu.VMEM(whole, BF16),
            pltpu.VMEM(whole, BF16),
            pltpu.VMEM(whole, BF16),
            pltpu.VMEM(whole, BF16),
            pltpu.VMEM(whole, BF16),
            pltpu.VMEM((3, 27, 8, 128), BF16),
            pltpu.VMEM((27, 8, 128), BF16),
            pltpu.VMEM((27, 8, 128), BF16),
            pltpu.VMEM((27, 8, 128), F32),
            pltpu.VMEM((27, 8, 128), F32),
            pltpu.VMEM((3, 2, 18, 16, 512), BF16),
            pltpu.VMEM((3, 4, 18, 16, 256), BF16),
            pltpu.VMEM((512, 512), BF16),
            pltpu.VMEM((2, 16, 16, 256), BF16),
            pltpu.VMEM((2, 256, 256), BF16),
            pltpu.VMEM((2, 256, 256), BF16),
            pltpu.VMEM((512, 512), F32),
            pltpu.VMEM((512, 256), F32),
            pltpu.VMEM((512, 512), F32),
            pltpu.VMEM((2, 16, 16, 512), BF16),
            pltpu.VMEM((2, 16, 16, 256), BF16),
            pltpu.VMEM((27, 8, 256), BF16),
            pltpu.SemaphoreType.DMA((COPIES,)),
            pltpu.SemaphoreType.DMA((COPIES,)),
            pltpu.SemaphoreType.DMA((4,)),
        ],
        compiler_params=pltpu.CompilerParams(
            collective_id=0, has_side_effects=True, vmem_limit_bytes=54_000_000
        ),
        cost_estimate=pl.CostEstimate(
            flops=11_000_000_000, bytes_accessed=4_000_000, transcendentals=1_000_000
        ),
    )(*(in_hbm(v) for v in (acts[0], cotangent[0], kernel.transpose(1, 0, 2))))
    outputs, grad_input, grad_kernel = pl.pallas_call(
        write_kernel,
        out_shape=results,
        in_specs=[vmem] * 3,
        out_specs=(vmem,) * 3,
        compiler_params=pltpu.CompilerParams(vmem_limit_bytes=8_000_000),
    )(*computed)
    return outputs[None], grad_input[None], grad_kernel.transpose(1, 0, 2)


def solution(mesh):
    return jax.shard_map(
        body,
        mesh=mesh,
        in_specs=(
            P("fsdp", "space", None, None, None),
            P("fsdp", None, None),
            P("fsdp", "space", None, None, None),
        ),
        out_specs=(
            P("fsdp", "space", None, None, None),
            P("fsdp", "space", None, None, None),
            P("fsdp", None, None),
        ),
        check_vma=False,
    )
```

```python
import jax
import jax.numpy as jnp
from jax import lax
from jax.experimental import pallas as pl
from jax.experimental.pallas import tpu as pltpu
from jax.sharding import PartitionSpec as P

MESH = pl.DeviceIdType.MESH
F32 = jnp.float32
BF16 = jnp.bfloat16
ORDERS = (("z", "x", "y"), ("y", "z", "x"), ("x", "y", "z"))
LOW, HIGH = pl.ds(0, 2), pl.ds(2, 2)
COPIES = 128


def silu(v):
    return v * jax.nn.sigmoid(v)


def step_kernel(
    acts_in,
    cot_in,
    shard_in,
    outputs,
    grad_input,
    grad_kernel,
    weights,
    partial,
    from_partner,
    rx3p,
    rx3m,
    rx2p,
    rx2m,
    rx1,
    own_sum,
    other_sum,
    final_own,
    final_other,
    hidden3,
    cot3,
    hidden_t,
    halo_cot,
    edge_out,
    edge_in,
    acc_edge,
    acc_mid,
    acc_back,
    acts,
    cot,
    shard,
    send_sem,
    recv_sem,
    local_sem,
):
    space, fsdp = lax.axis_index("space"), lax.axis_index("fsdp")
    core, z_hi = space % 2, space // 2
    y, x, zl = fsdp // 16, (fsdp // 4) % 4, fsdp % 4
    z = z_hi * 4 + zl
    own = {"y": y, "x": x, "z": zl}

    def neighbour(dim, delta):
        if dim == "y":
            return (space, ((y + 4 + delta) % 4) * 16 + x * 4 + zl)
        if dim == "x":
            return (space, y * 16 + ((x + 4 + delta) % 4) * 4 + zl)
        there = (z + 8 + delta) % 8
        return ((there // 4) * 2 + core, y * 16 + x * 4 + there % 4)

    partner = (z_hi * 2 + 1 - core, fsdp)
    across = ((space + 2) % 4, fsdp)
    greeted = [neighbour(d, k) for d in ("y", "x") for k in (1, -1, 2)]
    greeted += [neighbour("z", k) for k in (1, -1, 2, -2)]
    greeted += [partner, across, (3 - space, fsdp)]

    shard_copy = pltpu.make_async_copy(shard_in, shard, local_sem.at[1])
    cot_copy = pltpu.make_async_copy(cot_in, cot, local_sem.at[2])
    acts_copy = pltpu.make_async_copy(acts_in, acts, local_sem.at[3])
    shard_copy.start()
    cot_copy.start()
    acts_copy.start()

    barrier = pltpu.get_barrier_semaphore()
    for device in greeted:
        pl.semaphore_signal(barrier, inc=1, device_id=device, device_id_type=MESH)

    counter = [0]
    sent = []
    held = None

    def remote(src, dst, device):
        number = counter[0]
        counter[0] += 1
        return pltpu.make_async_remote_copy(
            src_ref=src,
            dst_ref=dst,
            send_sem=send_sem.at[number],
            recv_sem=recv_sem.at[number],
            device_id=device,
            device_id_type=MESH,
        )

    def send(src, dst, device):
        copy = remote(src, dst, device)
        if held is None:
            copy.start()
        else:
            held.append(copy)
        sent.append(copy)
        return copy

    def at(dim, delta):
        return (own[dim] + 4 + delta) % 4

    def place(colour, first, second, third):
        d1, d2, d3 = ORDERS[colour]
        index = {d1: first, d2: second, d3: third}
        return index["y"], index["x"], index["z"]

    every = slice(None)

    lanes = pl.ds(pl.multiple_of(core * 128, 128), 128)
    other_lanes = pl.ds(pl.multiple_of((1 - core) * 128, 128), 128)

    def down_copy(src, dst):
        return remote(src, dst, (space - 1, fsdp))

    def up_copy(src, dst):
        return remote(src, dst, (space + 1, fsdp))

    def when_low(action):
        pl.when(space > 0)(action)

    def when_high(action):
        pl.when(space < 3)(action)

    cot_down = down_copy(cot.at[0], halo_cot.at[1])
    cot_up = up_copy(cot.at[1], halo_cot.at[0])
    edge_down = down_copy(edge_out.at[0], edge_in.at[1])
    edge_up = up_copy(edge_out.at[1], edge_in.at[0])

    def slot(colour, first, second, third):
        iy, ix, iz = place(colour, first, second, third)
        return weights.at[core, pl.ds(9 * colour, 9), iy, ix, iz]

    waiting = {}

    def spread(key, colour, where, device):
        piece = slot(colour, *where)
        waiting.setdefault(key, []).append(send(piece, piece, device))

    def take(key):
        for copy in waiting.pop(key):
            copy.wait_recv()

    def gather_0(colour):
        d1, d2, d3 = ORDERS[colour]
        here = slot(colour, own[d1], own[d2], own[d3])
        for delta in (1, -1, 2):
            copy = send(shard.at[pl.ds(9 * colour, 9), :, lanes], here, neighbour(d1, delta))
            waiting.setdefault(f"a1{colour}", []).append(copy)

    def gather_1(colour):
        d1, d2, d3 = ORDERS[colour]
        for delta in (1, -1):
            spread(f"a2{colour}", colour, (every, own[d2], own[d3]), neighbour(d2, delta))

    def gather_2(colour):
        d1, d2, d3 = ORDERS[colour]
        take(f"a2{colour}")
        spread(f"a3{colour}", colour, (LOW, at(d2, -1), own[d3]), neighbour(d2, 1))
        spread(f"a3{colour}", colour, (HIGH, at(d2, 1), own[d3]), neighbour(d2, -1))

    def gather_3(colour):
        d1, d2, d3 = ORDERS[colour]
        take(f"a3{colour}")
        spread(f"a4{colour}", colour, (LOW, every, own[d3]), neighbour(d3, 1))
        spread(f"a4{colour}", colour, (HIGH, every, own[d3]), neighbour(d3, -1))
        spread(f"pair{colour}", colour, (every, every, own[d3]), partner)

    def gather_3b(colour):
        d1, d2, d3 = ORDERS[colour]
        spread(f"a5{colour}", colour, (HIGH, every, own[d3]), neighbour(d3, 1))
        spread(f"a5{colour}", colour, (LOW, every, own[d3]), neighbour(d3, -1))

    def gather_4(colour):
        d1, d2, d3 = ORDERS[colour]
        take(f"a4{colour}")
        spread(f"a5{colour}", colour, (LOW, every, at(d3, -1)), neighbour(d3, 1))
        spread(f"a5{colour}", colour, (HIGH, every, at(d3, 1)), neighbour(d3, -1))
        spread(f"pair{colour}", colour, (LOW, every, at(d3, -1)), partner)
        spread(f"pair{colour}", colour, (HIGH, every, at(d3, 1)), partner)

    def gather_5(colour):
        d1, d2, d3 = ORDERS[colour]
        take(f"a5{colour}")
        spread(f"pair{colour}", colour, (HIGH, every, at(d3, -1)), partner)
        spread(f"pair{colour}", colour, (LOW, every, at(d3, 1)), partner)
        spread(f"pair{colour}", colour, (every, every, at(d3, 2)), partner)

    def gather_6(colour):
        take(f"pair{colour}")

    def term(ref, colour, first, second, third, taps=None):
        iy, ix, iz = place(colour, first, second, third)
        taps = pl.ds(9 * colour, 9) if taps is None else taps
        if ref is partial:
            return (core, taps, iy, ix, iz)
        return (taps, iy, ix, iz)

    def pass_on(key, colour, where, dst, device):
        src = partial.at[term(partial, colour, *where)]
        copy = send(src, dst.at[term(dst, colour, *where)], device)
        waiting.setdefault(key, []).append(copy)

    def add(colour, where, *others):
        def one(tap, carry):
            tap = tap + 9 * colour
            mine = term(partial, colour, *where, taps=tap)
            total = partial[mine].astype(F32)
            for ref in others:
                total = total + ref[term(ref, colour, *where, taps=tap)].astype(F32)
            partial[mine] = total.astype(BF16)
            return carry

        lax.fori_loop(0, 9, one, 0)

    def reduce_pair(key, tap, count):
        taps = pl.ds(tap, count)
        copy = send(partial.at[1 - core, taps], from_partner.at[taps], partner)
        waiting.setdefault(key, []).append(copy)

    def reduce_phase(phase, part, colour):
        plus, minus = (rx3p, rx3m) if phase == 3 else (rx2p, rx2m)
        order = ORDERS[colour]
        dim = order[phase - 1]
        forward, backward = neighbour(dim, 1), neighbour(dim, -1)
        far, near = f"far{phase}{colour}", f"near{phase}{colour}"

        def where(half, delta):
            if phase == 3:
                return (half, every, at(dim, delta))
            return (half, at(dim, delta), own[order[2]])

        if part == "far":
            pass_on(far, colour, where(LOW, 2), plus, forward)
            pass_on(far, colour, where(HIGH, 2), minus, backward)
        elif part == "near":
            pass_on(near, colour, where(HIGH, 1), plus, forward)
            pass_on(near, colour, where(LOW, -1), minus, backward)
        elif part == 1:
            take(far)
            add(colour, where(LOW, 1), plus)
            pass_on(near, colour, where(LOW, 1), plus, forward)
            add(colour, where(HIGH, -1), minus)
            pass_on(near, colour, where(HIGH, -1), minus, backward)
        else:
            take(near)
            add(colour, where(every, 0), plus, minus)

    def reduce_1(colour):
        for key in ("p1",) if colour == 1 else ("p second",):
            if key in waiting:
                take(key)
        add(colour, (every, every, every), from_partner)
        reduce_phase(3, "far", colour)

    def reduce_1b(colour):
        reduce_phase(3, "near", colour)

    def reduce_2(colour):
        reduce_phase(3, 1, colour)

    def reduce_3(colour):
        reduce_phase(3, 2, colour)
        reduce_phase(2, "far", colour)
        reduce_phase(2, "near", colour)

    def reduce_4(colour):
        reduce_phase(2, 1, colour)

    def reduce_5(colour):
        reduce_phase(2, 2, colour)
        d1, d2, d3 = ORDERS[colour]
        for number, delta in enumerate((1, -1, 2)):
            src = partial.at[term(partial, colour, at(d1, delta), own[d2], own[d3])]
            dst = rx1.at[number, pl.ds(9 * colour, 9)]
            copy = send(src, dst, neighbour(d1, delta))
            waiting.setdefault(f"r6{colour}", []).append(copy)

    def reduce_6(colour):
        take(f"r6{colour}")
        for tap in range(9 * colour, 9 * colour + 9):
            total = partial[core, tap, y, x, zl].astype(F32)
            for number in range(3):
                total = total + rx1[number, tap].astype(F32)
            own_sum[tap] = total.astype(BF16)
        taps = pl.ds(9 * colour, 9)
        waiting[f"r7{colour}"] = [send(own_sum.at[taps], other_sum.at[taps], across)]

    def reduce_7(scale):
        for colour in range(3):
            take(f"r7{colour}")
        final_own[...] = (own_sum[...].astype(F32) + other_sum[...].astype(F32)) * scale
        waiting["r8"] = [send(final_own, final_other, partner)]
        grad_kernel[:, :, lanes] = final_own[...]

    def reduce_8():
        take("r8")
        grad_kernel[:, :, other_lanes] = final_other[...]

    def shifted(values):
        rows = values.shape[0]
        w = lax.broadcasted_iota(jnp.int32, values.shape, 0) % 16
        before = jnp.where(w == 0, 0.0, pltpu.roll(values, 1, axis=0))
        after = jnp.where(w == 15, 0.0, pltpu.roll(values, rows - 1, axis=0))
        return before.astype(BF16), values.astype(BF16), after.astype(BF16)

    def put_hidden(values, d, h, count):
        for number, part in enumerate(shifted(values)):
            hidden3[number, d, pl.ds(h, count)] = part.reshape(count, 16, 512)

    def put_cot(values, d, h, count):
        for number, part in enumerate(shifted(values)):
            cot3[2 - number, d, pl.ds(h, count)] = part.reshape(count, 16, 256)

    def prepare_cot():
        for ref, width in ((cot3, 256), (hidden3, 512)):
            edge = jnp.zeros((3, ref.shape[1], 16, width), BF16)
            ref[:, :, 0] = edge
            ref[:, :, 17] = edge

        def one(i, carry):
            d, h = i // 4, (i % 4) * 4
            values = cot[d, pl.ds(h, 4)].astype(F32).reshape(64, 256)
            put_cot(values, d + 1, h + 1, 4)
            return carry

        lax.fori_loop(0, 8, one, 0)

    def prepare_hidden():
        for i in range(4):
            d, h = i // 2, (i % 2) * 8
            values = silu(acts[d, pl.ds(h, 8)].astype(F32).reshape(128, 512))
            put_hidden(values, d, h + 1, 8)
            hidden_t[:, 128 * i : 128 * i + 128] = values.T.astype(BF16)

    def fill_halo(side):
        (cot_down if side else cot_up).wait_recv()

        def one(i, carry):
            values = halo_cot[side, pl.ds(i * 4, 4)].astype(F32).reshape(64, 256)
            put_cot(values, 3 * side, i * 4 + 1, 4)
            return carry

        lax.fori_loop(0, 4, one, 0)

    def fill_near():
        for side in range(2):
            pl.when(core == 1 - side)(lambda: fill_halo(side))

    def fill_far():
        pl.when(space == 1)(lambda: fill_halo(1))
        pl.when(space == 2)(lambda: fill_halo(0))

    def no_halo():
        for side in range(2):

            @pl.when(space == 3 * side)
            def _():
                cot3[:, 3 * side] = jnp.zeros((3, 18, 16, 256), BF16)
                edge_in[side] = jnp.zeros((256, 256), BF16)

    def cot_rows(colour, b, number):
        rows = cot3[number, pl.ds(2 - colour, 2), pl.ds(2 - b, 16)]
        return rows.reshape(512, 256)

    def kernel_term(colour, b):
        rows = [cot_rows(colour, b, number) for number in range(3)]
        product = jnp.dot(
            hidden_t[...], jnp.concatenate(rows, axis=1), preferred_element_type=F32
        )
        for number in range(3):
            for half in range(2):
                start = 256 * number + 128 * half
                part = product[:, start : start + 128].reshape(4, 4, 4, 8, 128)
                partial[half, 9 * colour + 3 * b + number] = part.astype(BF16)

    def tap_weight(tap):
        halves = [weights[half, tap].reshape(512, 128) for half in range(2)]
        return jnp.concatenate(halves, axis=1)

    def three_taps(colour, b):
        return [tap_weight(9 * colour + 3 * b + number) for number in range(3)]

    def hidden_rows(b):
        rows = [hidden3[number, :, pl.ds(b, 16)].reshape(512, 512) for number in range(3)]
        return jnp.concatenate(rows, axis=1)

    def add_back(colours, b, taps, first=False):
        grads = [cot_rows(colour, b, number) for colour in colours for number in range(3)]
        grads, taps = jnp.concatenate(grads, axis=1), jnp.concatenate(taps, axis=1)
        for start in (0, 256):
            product = lax.dot_general(
                grads,
                taps[start : start + 256],
                (((1,), (1,)), ((), ())),
                preferred_element_type=F32,
            )
            there = (slice(None), slice(start, start + 256))
            acc_back[there] = product if first else acc_back[there] + product

    def rows_of(d, b):
        rows = [hidden3[number, d, pl.ds(b, 16)].reshape(256, 512) for number in range(3)]
        return jnp.concatenate(rows, axis=1)

    def forward_part(b, below_d, above_d):
        for colour, d in ((0, below_d), (2, above_d)):
            product = jnp.dot(
                rows_of(d, b),
                jnp.concatenate(three_taps(colour, b), axis=0),
                preferred_element_type=F32,
            )
            there = (pl.ds(256 * d, 256), pl.ds(128 * colour, 256))
            acc_edge[there] = product if b == 0 else acc_edge[there] + product

    def forward_edges(b):
        forward_part(b, 1, 0)

    def forward_inner(b):
        forward_part(b, 0, 1)

    def back_edges(b):
        add_back((0, 2), b, three_taps(0, b) + three_taps(2, b), b == 0)

    def forward_and_back(b):
        taps = three_taps(1, b)
        weight = jnp.concatenate(taps, axis=0)
        for d in range(2):
            product = jnp.dot(rows_of(d, b), weight, preferred_element_type=F32)
            there = pl.ds(256 * d, 256)
            acc_mid[there] = product if b == 0 else acc_mid[there] + product
        add_back((1,), b, taps)

    def send_edges():
        edge_out[1] = acc_edge[256:, :256].astype(BF16)
        when_high(edge_up.start)
        edge_out[0] = acc_edge[:256, 256:].astype(BF16)
        when_low(edge_down.start)

    def write_outputs():
        when_low(edge_up.wait_recv)
        total = acc_mid[:256] + acc_edge[256:, 256:] + edge_in[0].astype(F32)
        outputs[0] = total.astype(BF16).reshape(16, 16, 256)
        when_high(edge_down.wait_recv)
        total = acc_mid[256:] + acc_edge[:256, :256] + edge_in[1].astype(F32)
        outputs[1] = total.astype(BF16).reshape(16, 16, 256)

    def write_grad_input():
        for i in range(8):
            d, h = i // 4, (i % 4) * 4
            values = acts[d, pl.ds(h, 4)].astype(F32).reshape(64, 512)
            squash = jax.nn.sigmoid(values)
            slope = squash * (1.0 + values * (1.0 - squash))
            total = acc_back[64 * i : 64 * i + 64] * slope
            grad_input[d, pl.ds(h, 4)] = total.astype(BF16).reshape(4, 16, 512)

    def finish():
        drain()

        @when_low
        def _():
            cot_down.wait_send()
            edge_down.wait_send()

        @when_high
        def _():
            cot_up.wait_send()
            edge_up.wait_send()

    def all_terms():
        nonlocal held
        held = []
        reduce_pair("p1", 9, 9)
        for colour in (1, 2, 0):
            gather_1(colour)
        middle, *second_sends = held
        held = None
        pieces = []
        base = counter[0]
        counter[0] += 6

        def piece(number, tap, count):
            taps = pl.ds(tap, count)
            return pltpu.make_async_remote_copy(
                src_ref=partial.at[1 - core, taps],
                dst_ref=from_partner.at[taps],
                send_sem=send_sem.at[base + number],
                recv_sem=recv_sem.at[base + number],
                device_id=partner,
                device_id_type=MESH,
            )

        def one(i, carry):
            group, b = i // 3, i % 3
            colour = 1 + ((group + 1) // 2) * (1 - 2 * z_hi) * (3 - 2 * group)

            @pl.when(i == 3)
            def _():
                middle.start()
                fill_near()

            @pl.when(i == 5)
            def _():
                mine.wait()
                for number, colour in enumerate((1, 2, 0)):
                    take(f"a1{colour}")
                    for copy in second_sends[2 * number : 2 * number + 2]:
                        copy.start()

            pl.when(i == 6)(fill_far)
            kernel_term(colour, b)

            @pl.when(i >= 3)
            def _():
                piece(i - 3, 9 * colour + 3 * b, 3).start()

            return carry

        lax.fori_loop(0, 9, one, 0)
        for number in range(6):
            tap = 9 * (2 - 2 * z_hi if number < 3 else 2 * z_hi) + 3 * (number % 3)
            pieces.append(piece(number, tap, 3))
        waiting["p second"] = pieces
        sent.extend(pieces)

    def drain():
        for copy in sent:
            copy.wait_send()
        sent.clear()

    pl.semaphore_wait(barrier, len(greeted))
    shard_copy.wait()
    gather_0(0)
    gather_0(1)
    gather_0(2)
    cot_copy.wait()
    when_low(cot_down.start)
    when_high(cot_up.start)
    mine = pltpu.make_async_copy(
        shard.at[:, :, lanes], weights.at[core, :, y, x, zl], local_sem.at[0]
    )
    mine.start()
    prepare_cot()
    acts_copy.wait()
    prepare_hidden()
    no_halo()
    all_terms()
    reduce_1(1)
    gather_2(2)
    gather_2(1)
    gather_2(0)
    reduce_1(0)
    reduce_1(2)
    reduce_1b(1)
    reduce_1b(0)
    reduce_1b(2)
    reduce_2(1)
    reduce_2(0)
    reduce_2(2)
    gather_3(2)
    gather_3(1)
    gather_3(0)
    reduce_3(1)
    reduce_3(0)
    reduce_3(2)
    gather_3b(2)
    gather_3b(1)
    gather_3b(0)
    gather_4(2)
    gather_4(1)
    gather_4(0)
    reduce_4(1)
    reduce_4(0)
    reduce_4(2)
    reduce_5(1)
    reduce_5(0)
    reduce_5(2)
    gather_5(2)
    gather_5(0)
    gather_5(1)
    gather_6(2)
    gather_6(0)
    forward_edges(0)
    forward_edges(1)
    forward_edges(2)
    reduce_6(1)
    reduce_6(0)
    reduce_6(2)
    send_edges()
    forward_inner(0)
    back_edges(0)
    forward_inner(1)
    back_edges(1)
    forward_inner(2)
    back_edges(2)
    gather_6(1)
    forward_and_back(0)
    forward_and_back(1)
    reduce_7(1.0 / lax.axis_size("fsdp"))
    forward_and_back(2)
    write_grad_input()
    drain()
    write_outputs()
    reduce_8()
    finish()


def write_kernel(outputs, grad_input, grad_kernel, outputs_to, grad_input_to, grad_kernel_to):
    outputs_to[...] = outputs[...]
    grad_input_to[...] = grad_input[...]
    grad_kernel_to[...] = grad_kernel[...]


def in_hbm(value):
    return pltpu.with_memory_space_constraint(value, pltpu.HBM)


def body(acts, kernel, cotangent):
    vmem = pl.BlockSpec(memory_space=pltpu.VMEM)
    whole = (27, 4, 4, 4, 8, 128)
    results = (
        jax.ShapeDtypeStruct((2, 16, 16, 256), BF16),
        jax.ShapeDtypeStruct((2, 16, 16, 512), BF16),
        jax.ShapeDtypeStruct((27, 8, 256), F32),
    )
    computed = pl.pallas_call(
        step_kernel,
        out_shape=results,
        in_specs=[pl.BlockSpec(memory_space=pltpu.HBM)] * 3,
        out_specs=(vmem,) * 3,
        scratch_shapes=[
            pltpu.VMEM((2, *whole), BF16),
            pltpu.VMEM((2, *whole), BF16),
            pltpu.VMEM(whole, BF16),
            pltpu.VMEM(whole, BF16),
            pltpu.VMEM(whole, BF16),
            pltpu.VMEM(whole, BF16),
            pltpu.VMEM(whole, BF16),
            pltpu.VMEM((3, 27, 8, 128), BF16),
            pltpu.VMEM((27, 8, 128), BF16),
            pltpu.VMEM((27, 8, 128), BF16),
            pltpu.VMEM((27, 8, 128), F32),
            pltpu.VMEM((27, 8, 128), F32),
            pltpu.VMEM((3, 2, 18, 16, 512), BF16),
            pltpu.VMEM((3, 4, 18, 16, 256), BF16),
            pltpu.VMEM((512, 512), BF16),
            pltpu.VMEM((2, 16, 16, 256), BF16),
            pltpu.VMEM((2, 256, 256), BF16),
            pltpu.VMEM((2, 256, 256), BF16),
            pltpu.VMEM((512, 512), F32),
            pltpu.VMEM((512, 256), F32),
            pltpu.VMEM((512, 512), F32),
            pltpu.VMEM((2, 16, 16, 512), BF16),
            pltpu.VMEM((2, 16, 16, 256), BF16),
            pltpu.VMEM((27, 8, 256), BF16),
            pltpu.SemaphoreType.DMA((COPIES,)),
            pltpu.SemaphoreType.DMA((COPIES,)),
            pltpu.SemaphoreType.DMA((4,)),
        ],
        compiler_params=pltpu.CompilerParams(
            collective_id=0, has_side_effects=True, vmem_limit_bytes=54_000_000
        ),
        cost_estimate=pl.CostEstimate(
            flops=11_000_000_000, bytes_accessed=4_000_000, transcendentals=1_000_000
        ),
    )(*(in_hbm(v) for v in (acts[0], cotangent[0], kernel.transpose(1, 0, 2))))
    outputs, grad_input, grad_kernel = pl.pallas_call(
        write_kernel,
        out_shape=results,
        in_specs=[vmem] * 3,
        out_specs=(vmem,) * 3,
        compiler_params=pltpu.CompilerParams(vmem_limit_bytes=8_000_000),
    )(*computed)
    return outputs[None], grad_input[None], grad_kernel.transpose(1, 0, 2)


def solution(mesh):
    return jax.shard_map(
        body,
        mesh=mesh,
        in_specs=(
            P("fsdp", "space", None, None, None),
            P("fsdp", None, None),
            P("fsdp", "space", None, None, None),
        ),
        out_specs=(
            P("fsdp", "space", None, None, None),
            P("fsdp", "space", None, None, None),
            P("fsdp", None, None),
        ),
        check_vma=False,
    )
```

```python
import jax
import jax.numpy as jnp
from jax import lax
from jax.experimental import pallas as pl
from jax.experimental.pallas import tpu as pltpu
from jax.sharding import PartitionSpec as P

MESH = pl.DeviceIdType.MESH
F32 = jnp.float32
BF16 = jnp.bfloat16
ORDERS = (("z", "x", "y"), ("y", "z", "x"), ("x", "y", "z"))
LOW, HIGH = pl.ds(0, 2), pl.ds(2, 2)
COPIES = 128


def silu(v):
    return v * jax.nn.sigmoid(v)


def step_kernel(
    acts_in,
    cot_in,
    shard_in,
    outputs,
    grad_input,
    grad_kernel,
    weights,
    partial,
    from_partner,
    rx3p,
    rx3m,
    rx2p,
    rx2m,
    rx1,
    own_sum,
    other_sum,
    final_own,
    final_other,
    hidden3,
    cot3,
    hidden_t,
    halo_cot,
    edge_out,
    edge_in,
    acc_edge,
    acc_mid,
    acc_back,
    acts,
    cot,
    shard,
    send_sem,
    recv_sem,
    local_sem,
):
    space, fsdp = lax.axis_index("space"), lax.axis_index("fsdp")
    core, z_hi = space % 2, space // 2
    y, x, zl = fsdp // 16, (fsdp // 4) % 4, fsdp % 4
    z = z_hi * 4 + zl
    own = {"y": y, "x": x, "z": zl}

    def neighbour(dim, delta):
        if dim == "y":
            return (space, ((y + 4 + delta) % 4) * 16 + x * 4 + zl)
        if dim == "x":
            return (space, y * 16 + ((x + 4 + delta) % 4) * 4 + zl)
        there = (z + 8 + delta) % 8
        return ((there // 4) * 2 + core, y * 16 + x * 4 + there % 4)

    partner = (z_hi * 2 + 1 - core, fsdp)
    across = ((space + 2) % 4, fsdp)
    greeted = [neighbour(d, k) for d in ("y", "x") for k in (1, -1, 2)]
    greeted += [neighbour("z", k) for k in (1, -1, 2, -2)]
    greeted += [partner, across, (3 - space, fsdp)]

    shard_copy = pltpu.make_async_copy(shard_in, shard, local_sem.at[1])
    cot_copy = pltpu.make_async_copy(cot_in, cot, local_sem.at[2])
    acts_copy = pltpu.make_async_copy(acts_in, acts, local_sem.at[3])
    shard_copy.start()
    cot_copy.start()
    acts_copy.start()

    barrier = pltpu.get_barrier_semaphore()
    for device in greeted:
        pl.semaphore_signal(barrier, inc=1, device_id=device, device_id_type=MESH)

    counter = [0]
    sent = []
    held = None

    def remote(src, dst, device):
        number = counter[0]
        counter[0] += 1
        return pltpu.make_async_remote_copy(
            src_ref=src,
            dst_ref=dst,
            send_sem=send_sem.at[number],
            recv_sem=recv_sem.at[number],
            device_id=device,
            device_id_type=MESH,
        )

    def send(src, dst, device):
        copy = remote(src, dst, device)
        if held is None:
            copy.start()
        else:
            held.append(copy)
        sent.append(copy)
        return copy

    def at(dim, delta):
        return (own[dim] + 4 + delta) % 4

    def place(colour, first, second, third):
        d1, d2, d3 = ORDERS[colour]
        index = {d1: first, d2: second, d3: third}
        return index["y"], index["x"], index["z"]

    every = slice(None)

    lanes = pl.ds(pl.multiple_of(core * 128, 128), 128)
    other_lanes = pl.ds(pl.multiple_of((1 - core) * 128, 128), 128)

    def down_copy(src, dst):
        return remote(src, dst, (space - 1, fsdp))

    def up_copy(src, dst):
        return remote(src, dst, (space + 1, fsdp))

    def when_low(action):
        pl.when(space > 0)(action)

    def when_high(action):
        pl.when(space < 3)(action)

    cot_down = down_copy(cot.at[0], halo_cot.at[1])
    cot_up = up_copy(cot.at[1], halo_cot.at[0])
    edge_down = down_copy(edge_out.at[0], edge_in.at[1])
    edge_up = up_copy(edge_out.at[1], edge_in.at[0])

    def slot(colour, first, second, third):
        iy, ix, iz = place(colour, first, second, third)
        return weights.at[core, pl.ds(9 * colour, 9), iy, ix, iz]

    waiting = {}

    def spread(key, colour, where, device):
        piece = slot(colour, *where)
        waiting.setdefault(key, []).append(send(piece, piece, device))

    def take(key):
        for copy in waiting.pop(key):
            copy.wait_recv()

    def gather_0(colour):
        d1, d2, d3 = ORDERS[colour]
        here = slot(colour, own[d1], own[d2], own[d3])
        for delta in (1, -1, 2):
            copy = send(shard.at[pl.ds(9 * colour, 9), :, lanes], here, neighbour(d1, delta))
            waiting.setdefault(f"a1{colour}", []).append(copy)

    def gather_1(colour):
        d1, d2, d3 = ORDERS[colour]
        for delta in (1, -1):
            spread(f"a2{colour}", colour, (every, own[d2], own[d3]), neighbour(d2, delta))

    def gather_2(colour):
        d1, d2, d3 = ORDERS[colour]
        take(f"a2{colour}")
        spread(f"a3{colour}", colour, (LOW, at(d2, -1), own[d3]), neighbour(d2, 1))
        spread(f"a3{colour}", colour, (HIGH, at(d2, 1), own[d3]), neighbour(d2, -1))

    def gather_3(colour):
        d1, d2, d3 = ORDERS[colour]
        take(f"a3{colour}")
        spread(f"a4{colour}", colour, (LOW, every, own[d3]), neighbour(d3, 1))
        spread(f"a4{colour}", colour, (HIGH, every, own[d3]), neighbour(d3, -1))
        spread(f"pair{colour}", colour, (every, every, own[d3]), partner)

    def gather_3b(colour):
        d1, d2, d3 = ORDERS[colour]
        spread(f"a5{colour}", colour, (HIGH, every, own[d3]), neighbour(d3, 1))
        spread(f"a5{colour}", colour, (LOW, every, own[d3]), neighbour(d3, -1))

    def gather_4(colour):
        d1, d2, d3 = ORDERS[colour]
        take(f"a4{colour}")
        spread(f"a5{colour}", colour, (LOW, every, at(d3, -1)), neighbour(d3, 1))
        spread(f"a5{colour}", colour, (HIGH, every, at(d3, 1)), neighbour(d3, -1))
        spread(f"pair{colour}", colour, (LOW, every, at(d3, -1)), partner)
        spread(f"pair{colour}", colour, (HIGH, every, at(d3, 1)), partner)

    def gather_5(colour):
        d1, d2, d3 = ORDERS[colour]
        take(f"a5{colour}")
        spread(f"pair{colour}", colour, (HIGH, every, at(d3, -1)), partner)
        spread(f"pair{colour}", colour, (LOW, every, at(d3, 1)), partner)
        spread(f"pair{colour}", colour, (every, every, at(d3, 2)), partner)

    def gather_6(colour):
        take(f"pair{colour}")

    def term(ref, colour, first, second, third, taps=None):
        iy, ix, iz = place(colour, first, second, third)
        taps = pl.ds(9 * colour, 9) if taps is None else taps
        if ref is partial:
            return (core, taps, iy, ix, iz)
        return (taps, iy, ix, iz)

    def pass_on(key, colour, where, dst, device):
        src = partial.at[term(partial, colour, *where)]
        copy = send(src, dst.at[term(dst, colour, *where)], device)
        waiting.setdefault(key, []).append(copy)

    def add(colour, where, *others):
        def one(tap, carry):
            tap = tap + 9 * colour
            mine = term(partial, colour, *where, taps=tap)
            total = partial[mine].astype(F32)
            for ref in others:
                total = total + ref[term(ref, colour, *where, taps=tap)].astype(F32)
            partial[mine] = total.astype(BF16)
            return carry

        lax.fori_loop(0, 9, one, 0)

    def reduce_pair(key, tap, count):
        taps = pl.ds(tap, count)
        copy = send(partial.at[1 - core, taps], from_partner.at[taps], partner)
        waiting.setdefault(key, []).append(copy)

    def reduce_phase(phase, part, colour):
        plus, minus = (rx3p, rx3m) if phase == 3 else (rx2p, rx2m)
        order = ORDERS[colour]
        dim = order[phase - 1]
        forward, backward = neighbour(dim, 1), neighbour(dim, -1)
        far, near = f"far{phase}{colour}", f"near{phase}{colour}"

        def where(half, delta):
            if phase == 3:
                return (half, every, at(dim, delta))
            return (half, at(dim, delta), own[order[2]])

        if part == "far":
            pass_on(far, colour, where(LOW, 2), plus, forward)
            pass_on(far, colour, where(HIGH, 2), minus, backward)
        elif part == "near":
            pass_on(near, colour, where(HIGH, 1), plus, forward)
            pass_on(near, colour, where(LOW, -1), minus, backward)
        elif part == 1:
            take(far)
            add(colour, where(LOW, 1), plus)
            pass_on(near, colour, where(LOW, 1), plus, forward)
            add(colour, where(HIGH, -1), minus)
            pass_on(near, colour, where(HIGH, -1), minus, backward)
        else:
            take(near)
            add(colour, where(every, 0), plus, minus)

    def reduce_1(colour):
        for key in ("p1",) if colour == 1 else ("p second",):
            if key in waiting:
                take(key)
        add(colour, (every, every, every), from_partner)
        reduce_phase(3, "far", colour)

    def reduce_1b(colour):
        reduce_phase(3, "near", colour)

    def reduce_2(colour):
        reduce_phase(3, 1, colour)

    def reduce_3(colour):
        reduce_phase(3, 2, colour)
        reduce_phase(2, "far", colour)
        reduce_phase(2, "near", colour)

    def reduce_4(colour):
        reduce_phase(2, 1, colour)

    def reduce_5(colour):
        reduce_phase(2, 2, colour)
        d1, d2, d3 = ORDERS[colour]
        for number, delta in enumerate((1, -1, 2)):
            src = partial.at[term(partial, colour, at(d1, delta), own[d2], own[d3])]
            dst = rx1.at[number, pl.ds(9 * colour, 9)]
            copy = send(src, dst, neighbour(d1, delta))
            waiting.setdefault(f"r6{colour}", []).append(copy)

    def reduce_6(colour):
        take(f"r6{colour}")
        for tap in range(9 * colour, 9 * colour + 9):
            total = partial[core, tap, y, x, zl].astype(F32)
            for number in range(3):
                total = total + rx1[number, tap].astype(F32)
            own_sum[tap] = total.astype(BF16)
        taps = pl.ds(9 * colour, 9)
        waiting[f"r7{colour}"] = [send(own_sum.at[taps], other_sum.at[taps], across)]

    def reduce_7(scale):
        for colour in range(3):
            take(f"r7{colour}")
        final_own[...] = (own_sum[...].astype(F32) + other_sum[...].astype(F32)) * scale
        waiting["r8"] = [send(final_own, final_other, partner)]
        grad_kernel[:, :, lanes] = final_own[...]

    def reduce_8():
        take("r8")
        grad_kernel[:, :, other_lanes] = final_other[...]

    def shifted(values):
        rows = values.shape[0]
        w = lax.broadcasted_iota(jnp.int32, values.shape, 0) % 16
        before = jnp.where(w == 0, 0.0, pltpu.roll(values, 1, axis=0))
        after = jnp.where(w == 15, 0.0, pltpu.roll(values, rows - 1, axis=0))
        return before.astype(BF16), values.astype(BF16), after.astype(BF16)

    def put_hidden(values, d, h, count):
        for number, part in enumerate(shifted(values)):
            hidden3[number, d, pl.ds(h, count)] = part.reshape(count, 16, 512)

    def put_cot(values, d, h, count):
        for number, part in enumerate(shifted(values)):
            cot3[2 - number, d, pl.ds(h, count)] = part.reshape(count, 16, 256)

    def prepare_cot():
        for ref, width in ((cot3, 256), (hidden3, 512)):
            edge = jnp.zeros((3, ref.shape[1], 16, width), BF16)
            ref[:, :, 0] = edge
            ref[:, :, 17] = edge

        def one(i, carry):
            d, h = i // 4, (i % 4) * 4
            values = cot[d, pl.ds(h, 4)].astype(F32).reshape(64, 256)
            put_cot(values, d + 1, h + 1, 4)
            return carry

        lax.fori_loop(0, 8, one, 0)

    def prepare_hidden():
        for i in range(4):
            d, h = i // 2, (i % 2) * 8
            values = silu(acts[d, pl.ds(h, 8)].astype(F32).reshape(128, 512))
            put_hidden(values, d, h + 1, 8)
            hidden_t[:, 128 * i : 128 * i + 128] = values.T.astype(BF16)

    def fill_halo(side):
        (cot_down if side else cot_up).wait_recv()

        def one(i, carry):
            values = halo_cot[side, pl.ds(i * 4, 4)].astype(F32).reshape(64, 256)
            put_cot(values, 3 * side, i * 4 + 1, 4)
            return carry

        lax.fori_loop(0, 4, one, 0)

    def fill_near():
        for side in range(2):
            pl.when(core == 1 - side)(lambda: fill_halo(side))

    def fill_far():
        pl.when(space == 1)(lambda: fill_halo(1))
        pl.when(space == 2)(lambda: fill_halo(0))

    def no_halo():
        for side in range(2):

            @pl.when(space == 3 * side)
            def _():
                cot3[:, 3 * side] = jnp.zeros((3, 18, 16, 256), BF16)
                edge_in[side] = jnp.zeros((256, 256), BF16)

    def cot_rows(colour, b, number):
        rows = cot3[number, pl.ds(2 - colour, 2), pl.ds(2 - b, 16)]
        return rows.reshape(512, 256)

    def kernel_term(colour, b):
        rows = [cot_rows(colour, b, number) for number in range(3)]
        rows = jnp.concatenate(rows, axis=1)
        for top in range(2):
            product = jnp.dot(
                hidden_t[256 * top : 256 * top + 256], rows, preferred_element_type=F32
            )
            for number in range(3):
                for half in range(2):
                    start = 256 * number + 128 * half
                    part = product[:, start : start + 128].reshape(2, 4, 4, 8, 128)
                    there = (half, 9 * colour + 3 * b + number, pl.ds(2 * top, 2))
                    partial[there] = part.astype(BF16)

    def tap_weight(tap):
        halves = [weights[half, tap].reshape(512, 128) for half in range(2)]
        return jnp.concatenate(halves, axis=1)

    def three_taps(colour, b):
        return [tap_weight(9 * colour + 3 * b + number) for number in range(3)]

    def hidden_rows(b):
        rows = [hidden3[number, :, pl.ds(b, 16)].reshape(512, 512) for number in range(3)]
        return jnp.concatenate(rows, axis=1)

    def add_back(colours, b, taps, first=False):
        grads = [cot_rows(colour, b, number) for colour in colours for number in range(3)]
        grads, taps = jnp.concatenate(grads, axis=1), jnp.concatenate(taps, axis=1)
        for start in (0, 256):
            product = lax.dot_general(
                grads,
                taps[start : start + 256],
                (((1,), (1,)), ((), ())),
                preferred_element_type=F32,
            )
            there = (slice(None), slice(start, start + 256))
            acc_back[there] = product if first else acc_back[there] + product

    def rows_of(d, b):
        rows = [hidden3[number, d, pl.ds(b, 16)].reshape(256, 512) for number in range(3)]
        return jnp.concatenate(rows, axis=1)

    def forward_part(b, below_d, above_d):
        for colour, d in ((0, below_d), (2, above_d)):
            product = jnp.dot(
                rows_of(d, b),
                jnp.concatenate(three_taps(colour, b), axis=0),
                preferred_element_type=F32,
            )
            there = (pl.ds(256 * d, 256), pl.ds(128 * colour, 256))
            acc_edge[there] = product if b == 0 else acc_edge[there] + product

    def forward_edges(b):
        forward_part(b, 1, 0)

    def forward_inner(b):
        forward_part(b, 0, 1)

    def back_edges(b):
        add_back((0, 2), b, three_taps(0, b) + three_taps(2, b), b == 0)

    def forward_and_back(b):
        taps = three_taps(1, b)
        weight = jnp.concatenate(taps, axis=0)
        for d in range(2):
            product = jnp.dot(rows_of(d, b), weight, preferred_element_type=F32)
            there = pl.ds(256 * d, 256)
            acc_mid[there] = product if b == 0 else acc_mid[there] + product
        add_back((1,), b, taps)

    def send_edges():
        edge_out[1] = acc_edge[256:, :256].astype(BF16)
        when_high(edge_up.start)
        edge_out[0] = acc_edge[:256, 256:].astype(BF16)
        when_low(edge_down.start)

    def write_outputs():
        when_low(edge_up.wait_recv)
        total = acc_mid[:256] + acc_edge[256:, 256:] + edge_in[0].astype(F32)
        outputs[0] = total.astype(BF16).reshape(16, 16, 256)
        when_high(edge_down.wait_recv)
        total = acc_mid[256:] + acc_edge[:256, :256] + edge_in[1].astype(F32)
        outputs[1] = total.astype(BF16).reshape(16, 16, 256)

    def write_grad_input():
        for i in range(8):
            d, h = i // 4, (i % 4) * 4
            values = acts[d, pl.ds(h, 4)].astype(F32).reshape(64, 512)
            squash = jax.nn.sigmoid(values)
            slope = squash * (1.0 + values * (1.0 - squash))
            total = acc_back[64 * i : 64 * i + 64] * slope
            grad_input[d, pl.ds(h, 4)] = total.astype(BF16).reshape(4, 16, 512)

    def finish():
        drain()

        @when_low
        def _():
            cot_down.wait_send()
            edge_down.wait_send()

        @when_high
        def _():
            cot_up.wait_send()
            edge_up.wait_send()

    def all_terms():
        nonlocal held
        held = []
        reduce_pair("p1", 9, 9)
        for colour in (1, 2, 0):
            gather_1(colour)
        middle, *second_sends = held
        held = None
        pieces = []
        base = counter[0]
        counter[0] += 6

        def piece(number, tap, count):
            taps = pl.ds(tap, count)
            return pltpu.make_async_remote_copy(
                src_ref=partial.at[1 - core, taps],
                dst_ref=from_partner.at[taps],
                send_sem=send_sem.at[base + number],
                recv_sem=recv_sem.at[base + number],
                device_id=partner,
                device_id_type=MESH,
            )

        def one(i, carry):
            group, b = i // 3, i % 3
            colour = 1 + ((group + 1) // 2) * (1 - 2 * z_hi) * (3 - 2 * group)

            @pl.when(i == 3)
            def _():
                middle.start()
                fill_near()

            @pl.when(i == 5)
            def _():
                mine.wait()
                for number, colour in enumerate((1, 2, 0)):
                    take(f"a1{colour}")
                    for copy in second_sends[2 * number : 2 * number + 2]:
                        copy.start()

            pl.when(i == 6)(fill_far)
            kernel_term(colour, b)

            @pl.when(i >= 3)
            def _():
                piece(i - 3, 9 * colour + 3 * b, 3).start()

            return carry

        lax.fori_loop(0, 9, one, 0)
        for number in range(6):
            tap = 9 * (2 - 2 * z_hi if number < 3 else 2 * z_hi) + 3 * (number % 3)
            pieces.append(piece(number, tap, 3))
        waiting["p second"] = pieces
        sent.extend(pieces)

    def drain():
        for copy in sent:
            copy.wait_send()
        sent.clear()

    pl.semaphore_wait(barrier, len(greeted))
    shard_copy.wait()
    gather_0(0)
    gather_0(1)
    gather_0(2)
    cot_copy.wait()
    when_low(cot_down.start)
    when_high(cot_up.start)
    mine = pltpu.make_async_copy(
        shard.at[:, :, lanes], weights.at[core, :, y, x, zl], local_sem.at[0]
    )
    mine.start()
    prepare_cot()
    acts_copy.wait()
    prepare_hidden()
    no_halo()
    all_terms()
    reduce_1(1)
    gather_2(2)
    gather_2(1)
    gather_2(0)
    reduce_1(0)
    reduce_1(2)
    reduce_1b(1)
    reduce_1b(0)
    reduce_1b(2)
    reduce_2(1)
    reduce_2(0)
    reduce_2(2)
    gather_3(2)
    gather_3(1)
    gather_3(0)
    reduce_3(1)
    reduce_3(0)
    reduce_3(2)
    gather_3b(2)
    gather_3b(1)
    gather_3b(0)
    gather_4(2)
    gather_4(1)
    gather_4(0)
    reduce_4(1)
    reduce_4(0)
    reduce_4(2)
    reduce_5(1)
    reduce_5(0)
    reduce_5(2)
    gather_5(2)
    gather_5(0)
    gather_5(1)
    gather_6(2)
    gather_6(0)
    forward_edges(0)
    forward_edges(1)
    forward_edges(2)
    reduce_6(1)
    reduce_6(0)
    reduce_6(2)
    send_edges()
    forward_inner(0)
    back_edges(0)
    forward_inner(1)
    back_edges(1)
    forward_inner(2)
    back_edges(2)
    gather_6(1)
    forward_and_back(0)
    forward_and_back(1)
    reduce_7(1.0 / lax.axis_size("fsdp"))
    forward_and_back(2)
    write_grad_input()
    drain()
    write_outputs()
    reduce_8()
    finish()


def write_kernel(outputs, grad_input, grad_kernel, outputs_to, grad_input_to, grad_kernel_to):
    outputs_to[...] = outputs[...]
    grad_input_to[...] = grad_input[...]
    grad_kernel_to[...] = grad_kernel[...]


def in_hbm(value):
    return pltpu.with_memory_space_constraint(value, pltpu.HBM)


def body(acts, kernel, cotangent):
    vmem = pl.BlockSpec(memory_space=pltpu.VMEM)
    whole = (27, 4, 4, 4, 8, 128)
    results = (
        jax.ShapeDtypeStruct((2, 16, 16, 256), BF16),
        jax.ShapeDtypeStruct((2, 16, 16, 512), BF16),
        jax.ShapeDtypeStruct((27, 8, 256), F32),
    )
    computed = pl.pallas_call(
        step_kernel,
        out_shape=results,
        in_specs=[pl.BlockSpec(memory_space=pltpu.HBM)] * 3,
        out_specs=(vmem,) * 3,
        scratch_shapes=[
            pltpu.VMEM((2, *whole), BF16),
            pltpu.VMEM((2, *whole), BF16),
            pltpu.VMEM(whole, BF16),
            pltpu.VMEM(whole, BF16),
            pltpu.VMEM(whole, BF16),
            pltpu.VMEM(whole, BF16),
            pltpu.VMEM(whole, BF16),
            pltpu.VMEM((3, 27, 8, 128), BF16),
            pltpu.VMEM((27, 8, 128), BF16),
            pltpu.VMEM((27, 8, 128), BF16),
            pltpu.VMEM((27, 8, 128), F32),
            pltpu.VMEM((27, 8, 128), F32),
            pltpu.VMEM((3, 2, 18, 16, 512), BF16),
            pltpu.VMEM((3, 4, 18, 16, 256), BF16),
            pltpu.VMEM((512, 512), BF16),
            pltpu.VMEM((2, 16, 16, 256), BF16),
            pltpu.VMEM((2, 256, 256), BF16),
            pltpu.VMEM((2, 256, 256), BF16),
            pltpu.VMEM((512, 512), F32),
            pltpu.VMEM((512, 256), F32),
            pltpu.VMEM((512, 512), F32),
            pltpu.VMEM((2, 16, 16, 512), BF16),
            pltpu.VMEM((2, 16, 16, 256), BF16),
            pltpu.VMEM((27, 8, 256), BF16),
            pltpu.SemaphoreType.DMA((COPIES,)),
            pltpu.SemaphoreType.DMA((COPIES,)),
            pltpu.SemaphoreType.DMA((4,)),
        ],
        compiler_params=pltpu.CompilerParams(
            collective_id=0, has_side_effects=True, vmem_limit_bytes=54_000_000
        ),
        cost_estimate=pl.CostEstimate(
            flops=11_000_000_000, bytes_accessed=4_000_000, transcendentals=1_000_000
        ),
    )(*(in_hbm(v) for v in (acts[0], cotangent[0], kernel.transpose(1, 0, 2))))
    outputs, grad_input, grad_kernel = pl.pallas_call(
        write_kernel,
        out_shape=results,
        in_specs=[vmem] * 3,
        out_specs=(vmem,) * 3,
        compiler_params=pltpu.CompilerParams(vmem_limit_bytes=8_000_000),
    )(*computed)
    return outputs[None], grad_input[None], grad_kernel.transpose(1, 0, 2)


def solution(mesh):
    return jax.shard_map(
        body,
        mesh=mesh,
        in_specs=(
            P("fsdp", "space", None, None, None),
            P("fsdp", None, None),
            P("fsdp", "space", None, None, None),
        ),
        out_specs=(
            P("fsdp", "space", None, None, None),
            P("fsdp", "space", None, None, None),
            P("fsdp", None, None),
        ),
        check_vma=False,
    )
```
